256 devices in a mesh: groups: 2 (over z), dap: 128 (over x, y, core).
Axes of the slice: x: 8, y: 8, z: 2, core: 2. Of those that a mesh axis runs over, the one named last changes fastest.
The devices are a block of a 8x8x16 slice.
Arguments:
- homolog_tensor: bfloat16 [1024, 256, 256], P(('groups', 'dap')), parts along dimension 0, may hold values from -1 to 1
- couple_tensor: bfloat16 [512, 256, 128], P(('groups', 'dap')), parts along dimension 0, may hold values from -6 to 6
- horizontal_drop_filter: int32 [512, 256], P('groups'), parts along dimension 0, may hold values 0 or 1
- couple_offset_matrix: bfloat16 [128, 8], replicated, may hold values from -0.29882812 to 0.29882812
- horizontal_attend_matrix: bfloat16 [256, 1024], replicated, may hold values from -0.375 to 0.375
- horizontal_exit_matrix: bfloat16 [256, 256], replicated, may hold values from -0.375 to 0.375
- vertical_attend_matrix: bfloat16 [256, 1024], replicated, may hold values from -0.375 to 0.375
- vertical_exit_matrix: bfloat16 [256, 256], replicated, may hold values from -0.375 to 0.375
- averaged_product_flanks: bfloat16 [256, 64], replicated, may hold values from -0.375 to 0.375
- averaged_product_exit: bfloat16 [1024, 128], replicated, may hold values from -1 to 1
Outputs:
- alignment_output: bfloat16 [1024, 256, 256], P('groups', 'dap'), parts along dimension 0
- pair_output_state: bfloat16 [512, 256, 128], P(('groups', 'dap')), parts along dimension 0
The draws below stay inside these ranges and needn't reach their ends.
There are 2 independent parts, one for each index of `groups`. The reference program is written for one: setup_inputs(seed, part) draws one part's arguments, and reference() takes and returns one part's arrays. A program takes and returns all parts, laid end to end along the dimension named above; an argument that names none is the same for every part. Nothing has to cross between parts.
All inputs are finite; a program needn't handle non-finite values.
Results may differ from the reference program's by a relative error of at most 0.012.
Values may be sent and summed in bfloat16 or wider, within the bound.
A program may use at most 64 MiB of HBM per device.

```python
import jax
import jax.numpy as jnp
from jax import lax

FEATURE_SIZE = 256
CZ = 128
HEAD_NUMBER = 8
HEAD_WIDTH = 32
FACTOR_FEATURES = 32
HOMOLOG_TOTAL = 512
AMINO_TOTAL = 256


def set_ends(result, stream_key, least, largest):
    longest = result.shape.index(max(result.shape))
    spots = []
    for shift in (0, 1):
        where = [jax.random.randint(jax.random.fold_in(stream_key, axis), (), 0, length) for axis, length in enumerate(result.shape)]
        where[longest] = (where[longest] + shift) % result.shape[longest]
        spots.append(tuple(where))
    return result.at[spots[0]].set(least).at[spots[1]].set(largest)


def level_of(rng, shape, cuts, least, largest):
    def one(position, parts):
        draws = jax.random.uniform(jax.random.fold_in(jax.random.fold_in(rng, 6), position), (parts,), jnp.float32, least / len(cuts), largest / len(cuts))
        return jnp.repeat(jnp.exp(draws), shape[position] // parts).reshape((-1,) + (1,) * (len(shape) - position - 1))

    factor_of = one(*cuts[0])
    for cut in cuts[1:]:
        factor_of = factor_of * one(*cut)
    return factor_of


def gaussian(own_key, shape, width, reach, split=(), kind=jnp.bfloat16):
    factor_of = level_of(own_key, shape, split, -0.22, 0.18) if split else 1.0
    result = jax.random.normal(own_key, shape, jnp.float32) * width * factor_of
    return jnp.minimum(jnp.maximum(result, -reach), reach).astype(kind)


def setup_inputs(seed: int = 0, part: int = 0) -> dict:
    splits = jax.random.split(jax.random.key(seed), 11)
    part_keys = jax.random.split(jax.random.fold_in(splits[10], part), 11)
    return {
        "homolog_tensor": gaussian(part_keys[0], (HOMOLOG_TOTAL, AMINO_TOTAL, FEATURE_SIZE), 0.2, 1.0, ((0, 128),)),
        "couple_tensor": gaussian(part_keys[1], (AMINO_TOTAL, AMINO_TOTAL, CZ), 1.0, 6.0, ((0, 128),)),
        "horizontal_drop_filter": set_ends((jax.random.randint(part_keys[2], (AMINO_TOTAL, FEATURE_SIZE), 0, 10) < 9).astype(jnp.int32), jax.random.fold_in(part_keys[2], 1), 0, 1),
        "couple_offset_matrix": gaussian(splits[3], (CZ, HEAD_NUMBER), 0.1, 0.29882812),
        "horizontal_attend_matrix": gaussian(splits[4], (FEATURE_SIZE, 4 * HEAD_NUMBER * HEAD_WIDTH), FEATURE_SIZE ** -0.5, 0.375),
        "horizontal_exit_matrix": gaussian(splits[5], (HEAD_NUMBER * HEAD_WIDTH, FEATURE_SIZE), (HEAD_NUMBER * HEAD_WIDTH) ** -0.5, 0.375),
        "vertical_attend_matrix": gaussian(splits[6], (FEATURE_SIZE, 4 * HEAD_NUMBER * HEAD_WIDTH), FEATURE_SIZE ** -0.5, 0.375),
        "vertical_exit_matrix": gaussian(splits[7], (HEAD_NUMBER * HEAD_WIDTH, FEATURE_SIZE), (HEAD_NUMBER * HEAD_WIDTH) ** -0.5, 0.375),
        "averaged_product_flanks": gaussian(splits[8], (FEATURE_SIZE, 2 * FACTOR_FEATURES), FEATURE_SIZE ** -0.5, 0.375),
        "averaged_product_exit": gaussian(splits[9], (FACTOR_FEATURES * FACTOR_FEATURES, CZ), FACTOR_FEATURES ** -0.5, 1.0),
    }


def standardise_features(values):
    values = values.astype(jnp.float32)
    center = values - lax.optimization_barrier(jnp.mean(values, axis=-1, keepdims=True))
    spread = lax.optimization_barrier(jnp.mean(center * center, axis=-1, keepdims=True))
    return center * lax.rsqrt(spread + 1e-05)

def attend(normed, w_qkvg, w_out, bias):
    batch, length = (normed.shape[0], normed.shape[1])
    proj = jnp.einsum('blc,cf->blf', normed.astype(jnp.float32), w_qkvg.astype(jnp.float32))
    proj = proj.reshape(batch, length, 4, HEAD_NUMBER, HEAD_WIDTH)
    query = (proj[:, :, 0] * HEAD_WIDTH ** (-0.5)).astype(jnp.bfloat16)
    keys = proj[:, :, 1].astype(jnp.bfloat16)
    values = proj[:, :, 2].astype(jnp.bfloat16)
    gate = proj[:, :, 3]
    if bias is None:
        bias = jnp.zeros((HEAD_NUMBER, length, length), jnp.bfloat16)

    def one_head(items):
        qh, kh, vh, bh = items
        scores = jnp.einsum('bid,bjd->bij', qh.astype(jnp.float32), kh.astype(jnp.float32))
        scores = scores + bh.astype(jnp.float32)[None]
        weights = jax.nn.softmax(scores, axis=-1).astype(jnp.bfloat16)
        return jnp.einsum('bij,bjd->bid', weights.astype(jnp.float32), vh.astype(jnp.float32))
    heads = lax.map(one_head, (jnp.moveaxis(query, 2, 0), jnp.moveaxis(keys, 2, 0), jnp.moveaxis(values, 2, 0), bias))
    heads = jnp.moveaxis(heads, 0, 2)
    gated = (jax.nn.sigmoid(gate) * heads).astype(jnp.bfloat16).reshape(batch, length, HEAD_NUMBER * HEAD_WIDTH)
    return jnp.einsum('blk,kc->blc', gated.astype(jnp.float32), w_out.astype(jnp.float32))

def reference(homolog_tensor, couple_tensor, horizontal_drop_filter, couple_offset_matrix, horizontal_attend_matrix, horizontal_exit_matrix, vertical_attend_matrix, vertical_exit_matrix, averaged_product_flanks, averaged_product_exit):
    normed_pair = standardise_features(couple_tensor).astype(jnp.bfloat16)
    bias = jnp.einsum('ijz,zh->hij', normed_pair.astype(jnp.float32), couple_offset_matrix.astype(jnp.float32)).astype(jnp.bfloat16)
    starting_answer = standardise_features(homolog_tensor).astype(jnp.bfloat16)
    perform_refresh = attend(starting_answer, horizontal_attend_matrix, horizontal_exit_matrix, bias)
    homolog_later = (homolog_tensor.astype(jnp.float32) + horizontal_drop_filter.astype(jnp.float32) * (1.0 / 0.9) * perform_refresh).astype(jnp.bfloat16)
    column_layout = jnp.swapaxes(homolog_later, 0, 1)
    perform_refresh = attend(standardise_features(column_layout).astype(jnp.bfloat16), vertical_attend_matrix, vertical_exit_matrix, None)
    alignment_output = jnp.swapaxes((column_layout.astype(jnp.float32) + perform_refresh).astype(jnp.bfloat16), 0, 1)
    final_result = standardise_features(alignment_output).astype(jnp.bfloat16)
    factors = jnp.einsum('sic,cf->sif', final_result.astype(jnp.float32), averaged_product_flanks.astype(jnp.float32))
    left = factors[..., :FACTOR_FEATURES].astype(jnp.bfloat16)
    right = factors[..., FACTOR_FEATURES:].astype(jnp.bfloat16)

    def one_row(items):
        left_row, pair_row = items
        outer = jnp.einsum('sc,sjd->jcd', left_row.astype(jnp.float32), right.astype(jnp.float32)) / HOMOLOG_TOTAL
        outer = outer.astype(jnp.bfloat16).reshape(AMINO_TOTAL, FACTOR_FEATURES * FACTOR_FEATURES)
        change = jnp.dot(outer, averaged_product_exit, preferred_element_type=jnp.float32)
        return (pair_row.astype(jnp.float32) + change).astype(jnp.bfloat16)
    pair_output_state = lax.map(one_row, (jnp.swapaxes(left, 0, 1), couple_tensor))
    return (alignment_output, pair_output_state)
```

```python
import jax
import jax.numpy as jnp
from jax import lax
from jax.experimental import pallas as pl
from jax.experimental.pallas import tpu as pltpu
from jax.sharding import Mesh
from jax.sharding import PartitionSpec as P

HEADS = 8
WIDTH = 32
FACTORS = 32
NX, NY, NC = 8, 8, 2
LANES = 128
GROUPS_DAP = ("groups", "dap_0", "dap_1", "dap_2")
DAP = ("dap_0", "dap_1", "dap_2")
MESH = pl.DeviceIdType.MESH
F32, BF16 = jnp.float32, jnp.bfloat16
VMEM = pl.BlockSpec(memory_space=pltpu.VMEM)
LIMIT = 60 * 1024 * 1024
RING_ORDER = (4, 3, 5, 2, 6, 1, 7)


def norm(v):
    center = v - jnp.mean(v, axis=-1, keepdims=True)
    spread = jnp.mean(center * center, axis=-1, keepdims=True)
    return center * lax.rsqrt(spread + 1e-05)


def nt(a, b):
    return lax.dot_general(a, b, (((1,), (1,)), ((), ())), preferred_element_type=F32)


def nn(a, b):
    return jnp.dot(a, b, preferred_element_type=F32)


def here():
    return lax.axis_index("dap_0"), lax.axis_index("dap_1"), lax.axis_index("dap_2")


def place(x, y, c):
    return {"dap_0": x, "dap_1": y, "dap_2": c}


def greet(peers):
    sem = pltpu.get_barrier_semaphore()
    for peer in peers:
        pl.semaphore_signal(sem, inc=1, device_id=peer, device_id_type=MESH)
    pl.semaphore_wait(sem, len(peers))


def x_peers(x, y, c):
    return [place((x + k) % NX, y, c) for k in RING_ORDER]


def y_peers(x, y, c):
    return [place(x, (y + k) % NY, c) for k in RING_ORDER]


def push(src, dst, send, recv, peer):
    copy = pltpu.make_async_remote_copy(
        src_ref=src, dst_ref=dst, send_sem=send, recv_sem=recv, device_id=peer, device_id_type=MESH
    )
    copy.start()
    return copy


def keep(src, dst, sem):
    copy = pltpu.make_async_copy(src, dst, sem)
    copy.start()
    return copy


def wide_y(x, y, c):
    out = [(NY * NC - 2, place(x, y, 1 - c), y, 1 - c)]
    for k in RING_ORDER:
        for f in range(NC):
            cc = (c + f) % NC
            yy = (y + k) % NY
            out.append((2 * (k - 1) + f, place(x, yy, cc), yy, cc))
    return out


def wide_x(x, y, c):
    out = [(NX * NC - 2, place(x, y, 1 - c), x, 1 - c)]
    for k in RING_ORDER:
        for f in range(NC):
            cc = (c + f) % NC
            xx = (x + k) % NX
            out.append((2 * (k - 1) + f, place(xx, y, cc), xx, cc))
    return out


def bias_rows_kernel(pair_ref, w_ref, out_ref):
    zn = norm(pair_ref[...].astype(F32)).astype(BF16)
    rows = nt(w_ref[...], zn)
    length = rows.shape[1] // 2
    both = jnp.concatenate([rows[:, :length], rows[:, length:]], axis=0).astype(BF16)
    for k in range(2):
        out_ref[k] = both[:, k * LANES : (k + 1) * LANES]


def bias_gather_kernel(
    own, full, keep_sem, s0, r0, s1, r1, s2, r2, s3, r3, s4, r4, s5, r5
):
    x, y, c = here()
    yc = y * NC + c
    mine = [keep(own.at[k], full.at[k, x, yc], keep_sem.at[k]) for k in range(2)]
    wy, wx = wide_y(x, y, c), wide_x(x, y, c)
    greet([p for _, p, _, _ in wy] + [p for _, p, _, _ in wx[1:]])
    first0 = [push(own.at[0], full.at[0, x, yc], s0.at[n], r0.at[n], p) for n, p, _, _ in wy]
    first1 = [push(own.at[1], full.at[1, x, yc], s1.at[n], r1.at[n], p) for n, p, _, _ in wx]
    for m in mine:
        m.wait()
    for m in first0:
        m.wait_recv()
    half = pl.ds(c * NY, NY)
    second0 = [
        push(full.at[0, x, half], full.at[0, x, half], s2.at[k - 1], r2.at[k - 1], place((x + k) % NX, y, c))
        for k in RING_ORDER
    ]
    for m in first1:
        m.wait_recv()
    halfx, pair = pl.ds(c * (NX // 2), NX // 2), pl.ds(y * NC, NC)
    second1 = [
        push(full.at[1, halfx, pair], full.at[1, halfx, pair], s3.at[k - 1], r3.at[k - 1], place(x, (y + k) % NY, c))
        for k in RING_ORDER
    ]
    other = place(x, y, 1 - c)
    third = []
    for n in reversed(range(NX - 1)):
        k = RING_ORDER[n]
        second0[n].wait_recv()
        xs = (x + NX - k) % NX
        third.append(push(full.at[0, xs, half], full.at[0, xs, half], s4.at[k - 1], r4.at[k - 1], other))
        second1[n].wait_recv()
        pairs = pl.ds(((y + NY - k) % NY) * NC, NC)
        third.append(push(full.at[1, halfx, pairs], full.at[1, halfx, pairs], s5.at[k - 1], r5.at[k - 1], other))
    for m in third:
        m.wait_recv()
    for m in first0 + first1 + second0 + second1 + third:
        m.wait_send()


def heads_of(q_ref, k_ref, v_ref, rows, bias_of):
    length = k_ref.shape[0]
    lane = lax.broadcasted_iota(jnp.int32, (1, LANES), 1) // WIDTH
    per = LANES // WIDTH
    out = []
    for t in range(HEADS // per):
        tile = slice(t * LANES, (t + 1) * LANES)
        total = None
        for e in range(per):
            h = t * per + e
            mask = (lane == e).astype(F32).astype(BF16)
            scores = nt(q_ref[rows, tile] * mask, k_ref[:, tile])
            if bias_of is not None:
                scores = scores + bias_of(h)
            top = jnp.max(scores, axis=-1, keepdims=True)
            raised = jnp.exp(scores - top)
            scale = 1.0 / jnp.sum(raised, axis=-1, keepdims=True)
            weights = (raised * scale).astype(BF16)
            part = nn(weights, v_ref[:, tile] * mask)
            total = part if total is None else total + part
        out.append(total)
    return out


def row_kernel(msa_ref, bias_ref, drop_ref, w_ref, wo_ref, out_ref, wide, bias, q, k, v, g, res, stage):
    seqs, length, width = msa_ref.shape
    pairs = length // 2
    for t in range(2):
        wide[t] = bias_ref[t].astype(F32).reshape(length * HEADS, LANES)
    for h in range(HEADS):
        for t in range(2):
            tile = slice(t * LANES, (t + 1) * LANES)
            bias[h, :, tile] = wide[t, pl.ds(h, length, stride=HEADS), :]

    def one(s, carry):
        token = msa_ref[s].astype(F32)
        m1 = norm(token).astype(BF16)
        q[...] = (nn(m1, w_ref[:, 0:width]) * WIDTH ** (-0.5)).astype(BF16)
        k[...] = nn(m1, w_ref[:, width : 2 * width]).astype(BF16)
        v[...] = nn(m1, w_ref[:, 2 * width : 3 * width]).astype(BF16)
        g[...] = nn(m1, w_ref[:, 3 * width : 4 * width])
        heads = jnp.concatenate(heads_of(q, k, v, slice(None), lambda h: bias[h]), axis=-1)
        gated = (jax.nn.sigmoid(g[...]) * heads).astype(BF16)
        change = nn(gated, wo_ref[...])
        after = token + drop_ref[...].astype(F32) * (1.0 / 0.9) * change
        for t in range(2):
            res[t] = after[:, t * LANES : (t + 1) * LANES]
            for r in range(2):
                stage[t, pl.ds(s * 2 + r, pairs, stride=seqs * 2), :] = res[t, pl.ds(r, pairs, stride=2), :]
        return carry

    lax.fori_loop(0, seqs, one, 0)
    for t in range(2):
        out_ref[t] = stage[t].reshape(out_ref.shape[1:]).astype(BF16)


def exchange_kernel(src, dst, mid0, mid1, keep_sem, s0, r0, s1, r1, s2, r2, s3, r3):
    x, y, c = here()
    yc = y * NC + c
    a = keep(src.at[0, x], mid0.at[x], keep_sem.at[0])
    b = keep(src.at[1, :, yc], mid1.at[yc], keep_sem.at[1])
    wy = wide_y(x, y, c)
    greet([p for _, p, _, _ in wy] + x_peers(x, y, c))
    first0 = [
        push(src.at[0, (x + k) % NX], mid0.at[x], s0.at[k - 1], r0.at[k - 1], place((x + k) % NX, y, c))
        for k in RING_ORDER
    ]
    first1 = [
        push(src.at[1, :, yy * NC + cc], mid1.at[yc], s1.at[n], r1.at[n], p) for n, p, yy, cc in wy
    ]
    a.wait()
    b.wait()
    for m in first0:
        m.wait_recv()
    second0 = [
        push(mid0.at[:, yy * NC + cc], dst.at[0, :, yc], s2.at[n], r2.at[n], p) for n, p, yy, cc in wy
    ]
    a = keep(mid0.at[:, yc], dst.at[0, :, yc], keep_sem.at[0])
    for m in first1:
        m.wait_recv()
    second1 = [
        push(mid1.at[:, (x + k) % NX], dst.at[1, x], s3.at[k - 1], r3.at[k - 1], place((x + k) % NX, y, c))
        for k in RING_ORDER
    ]
    b = keep(mid1.at[:, x], dst.at[1, x], keep_sem.at[1])
    a.wait()
    b.wait()
    for m in second0 + second1:
        m.wait_recv()
    for m in first0 + first1 + second0 + second1:
        m.wait_send()


def column_kernel(in_ref, w_ref, wo_ref, flank_ref, out_ref, left_ref, right_ref, both, q, k, v, g, acc):
    width = w_ref.shape[0]
    tokens = out_ref.shape[0]
    seqs = tokens // 2
    for t in range(2):
        both[t] = in_ref[t].astype(F32).reshape(tokens, LANES)

    def one(r, carry):
        token = jnp.concatenate([both[t, pl.ds(r, seqs, stride=2), :] for t in range(2)], axis=-1)
        m3 = norm(token).astype(BF16)
        q[...] = (nn(m3, w_ref[:, 0:width]) * WIDTH ** (-0.5)).astype(BF16)
        k[...] = nn(m3, w_ref[:, width : 2 * width]).astype(BF16)
        v[...] = nn(m3, w_ref[:, 2 * width : 3 * width]).astype(BF16)
        g[...] = nn(m3, w_ref[:, 3 * width : 4 * width])
        step = 256

        def chunk(n, inner):
            rows = pl.ds(pl.multiple_of(n * step, step), step)
            heads = jnp.concatenate(heads_of(q, k, v, rows, None), axis=-1)
            acc[rows, :] = (jax.nn.sigmoid(g[rows, :]) * heads).astype(BF16)
            return inner

        lax.fori_loop(0, seqs // step, chunk, 0)
        after = (token + nn(acc[...], wo_ref[...])).astype(BF16).astype(F32)
        for t in range(2):
            both[t, pl.ds(r, seqs, stride=2), :] = after[:, t * LANES : (t + 1) * LANES]
        m4 = norm(after).astype(BF16)
        factors = nt(flank_ref[...], m4).astype(BF16)
        left_ref[r] = factors[:FACTORS]
        right_ref[r] = factors[FACTORS:]
        return carry

    lax.fori_loop(0, 2, one, 0)
    for t in range(2):
        out_ref[:, t * LANES : (t + 1) * LANES] = both[t].astype(BF16)


def outer_kernel(
    left, right, exit_ref, change, lefts, rights, others, prod, wide, diag, tile, arrive, land,
    keep_sem, s0, r0, s1, r1, s2, r2, s3, r3,
):
    x, y, c = here()
    own = [keep(left, lefts.at[y], keep_sem.at[0]), keep(right, rights.at[x], keep_sem.at[1])]
    other = place(x, y, 1 - c)
    greet(y_peers(x, y, c) + x_peers(x, y, c) + [other])
    fl = [
        push(left, lefts.at[y], s0.at[k - 1], r0.at[k - 1], place(x, (y + k) % NY, c)) for k in RING_ORDER
    ]
    fr = [
        push(right, rights.at[x], s1.at[k - 1], r1.at[k - 1], place((x + k) % NX, y, c)) for k in RING_ORDER
    ]
    swap = [push(right, others.at[x], s2.at[NX - 1], r2.at[NX - 1], other)]

    depth = exit_ref.shape[1]
    per = LANES // FACTORS
    wide[...] = exit_ref[...].astype(F32)
    diag[...] = jnp.zeros_like(diag)
    for d in range(FACTORS):
        block = wide[pl.ds(d, FACTORS, stride=FACTORS), :].astype(BF16)
        for e in range(per):
            diag[d, e * FACTORS : (e + 1) * FACTORS, e * depth : (e + 1) * depth] = block

    for n in reversed(range(NX - 1)):
        k = RING_ORDER[n]
        fr[n].wait_recv()
        xs = (x + NX - k) % NX
        swap.append(push(rights.at[xs], others.at[xs], s2.at[k - 1], r2.at[k - 1], other))
    for m in own:
        m.wait()
    for m in fl:
        m.wait_recv()

    seqs = left.shape[1]
    rows = rights.shape[0] * rights.shape[1]
    js = rows // FACTORS
    pitch = FACTORS + 8
    cols = lefts[...].reshape(lefts.shape[0] * lefts.shape[1], seqs)
    lots = cols.shape[0] // LANES

    def fill(source, base):
        both = source[...].reshape(rows, seqs)
        out = nt(both, cols) * (1.0 / seqs)
        for n in range(js):
            for u in range(lots):
                at = pl.ds(pl.multiple_of((base + n) * pitch, 8), FACTORS)
                prod[u, at, :] = out[n * FACTORS : (n + 1) * FACTORS, u * LANES : (u + 1) * LANES]

    fill(rights, c * js)
    for m in swap:
        m.wait_recv()
    fill(others, (1 - c) * js)
    for e in range(per):
        tile[e] = jnp.zeros(tile.shape[1:], F32)

    def step(d, carry):
        lhs = jnp.concatenate(
            [prod[u, pl.ds(d, 2 * js, stride=pitch), :] for u in range(lots)], axis=0
        ).astype(BF16)
        add = nn(lhs, diag[d])
        for e in range(per):
            tile[e, : lots * 2 * js, :] += add[:, e * depth : (e + 1) * depth]
        return carry

    lax.fori_loop(0, FACTORS, step, 0)
    for u in range(lots):
        for e in range(per):
            i = u * per + e
            arrive[i // 2, i % 2] = tile[e, u * 2 * js : (u + 1) * 2 * js, :].astype(BF16)
    own = keep(arrive.at[y], land.at[y], keep_sem.at[0])
    back = [
        push(arrive.at[(y + k) % NY], land.at[y], s3.at[k - 1], r3.at[k - 1], place(x, (y + k) % NY, c))
        for k in RING_ORDER
    ]
    own.wait()
    for m in back:
        m.wait_recv()
    for t in range(2):
        for yy in range(NY):
            tile[t, yy * 2 * js : (yy + 1) * 2 * js, :] = land[yy, t].astype(F32)
            for cc in range(NC):
                for r in range(2):
                    change[t, pl.ds((yy * NC + cc) * 2 + r, NX, stride=NY * NC * 2), :] = tile[
                        t, pl.ds(yy * 2 * js + cc * js + r, NX, stride=2), :
                    ]
    for m in fl + fr + swap + back:
        m.wait_send()


def sems(*counts):
    out = []
    for n in counts:
        out += [pltpu.SemaphoreType.DMA((n,)), pltpu.SemaphoreType.DMA((n,))]
    return out


def remote(number):
    return pltpu.CompilerParams(collective_id=number, has_side_effects=True, vmem_limit_bytes=LIMIT)


def shards(msa, pair, drop, w_bias, w_row, wo_row, w_col, wo_col, flanks, w_exit):
    seqs, length, width = msa.shape
    rows, _, depth = pair.shape
    everyone = NX * NY * NC
    wide = NY * NC - 1
    local = pltpu.CompilerParams(vmem_limit_bytes=LIMIT)
    own = pl.pallas_call(
        bias_rows_kernel,
        out_shape=jax.ShapeDtypeStruct((2, rows * HEADS, LANES), BF16),
        in_specs=[VMEM] * 2,
        out_specs=VMEM,
        compiler_params=local,
    )(pair.reshape(rows * length, depth), w_bias.T)
    bias = pl.pallas_call(
        bias_gather_kernel,
        out_shape=jax.ShapeDtypeStruct((2, NX, NY * NC, rows * HEADS, LANES), BF16),
        in_specs=[VMEM],
        out_specs=VMEM,
        scratch_shapes=[pltpu.SemaphoreType.DMA((2,))]
        + sems(wide, wide, NX - 1, NY - 1, NX - 1, NY - 1),
        compiler_params=remote(0),
    )(own)
    msa2 = pl.pallas_call(
        row_kernel,
        out_shape=jax.ShapeDtypeStruct((2, NX, NY * NC, seqs * rows, LANES), BF16),
        in_specs=[VMEM] * 5,
        out_specs=VMEM,
        scratch_shapes=[
            pltpu.VMEM((2, length * HEADS, LANES), F32),
            pltpu.VMEM((HEADS, length, length), F32),
            pltpu.VMEM((length, width), BF16),
            pltpu.VMEM((length, width), BF16),
            pltpu.VMEM((length, width), BF16),
            pltpu.VMEM((length, width), F32),
            pltpu.VMEM((2, length, LANES), F32),
            pltpu.VMEM((2, seqs * length, LANES), F32),
        ],
        compiler_params=local,
    )(msa, bias, drop, w_row, wo_row)
    turned = pl.pallas_call(
        exchange_kernel,
        out_shape=jax.ShapeDtypeStruct(msa2.shape, BF16),
        in_specs=[VMEM],
        out_specs=VMEM,
        scratch_shapes=[
            pltpu.VMEM((NX, NY * NC, seqs * rows, LANES), BF16),
            pltpu.VMEM((NY * NC, NX, seqs * rows, LANES), BF16),
            pltpu.SemaphoreType.DMA((2,)),
        ]
        + sems(NX - 1, wide, wide, NX - 1),
        compiler_params=remote(1),
    )(msa2)
    total = seqs * everyone
    aligned, left, right = pl.pallas_call(
        column_kernel,
        out_shape=(
            jax.ShapeDtypeStruct((total * rows, width), BF16),
            jax.ShapeDtypeStruct((rows, FACTORS, total), BF16),
            jax.ShapeDtypeStruct((rows, FACTORS, total), BF16),
        ),
        in_specs=[VMEM] * 4,
        out_specs=(VMEM,) * 3,
        scratch_shapes=[
            pltpu.VMEM((2, total * rows, LANES), F32),
            pltpu.VMEM((total, width), BF16),
            pltpu.VMEM((total, width), BF16),
            pltpu.VMEM((total, width), BF16),
            pltpu.VMEM((total, width), F32),
            pltpu.VMEM((total, width), BF16),
        ],
        compiler_params=local,
    )(turned, w_col, wo_col, flanks.T)
    chunk = (rows * FACTORS, total)
    js = NX * rows
    lots = NY * rows * FACTORS // LANES
    change = pl.pallas_call(
        outer_kernel,
        out_shape=jax.ShapeDtypeStruct(pair.shape, F32),
        in_specs=[VMEM] * 3,
        out_specs=VMEM,
        scratch_shapes=[
            pltpu.VMEM((NY,) + chunk, BF16),
            pltpu.VMEM((NX,) + chunk, BF16),
            pltpu.VMEM((NX,) + chunk, BF16),
            pltpu.VMEM((lots, 2 * js * (FACTORS + 8), LANES), F32),
            pltpu.VMEM(w_exit.shape, F32),
            pltpu.VMEM((FACTORS, LANES, (LANES // FACTORS) * depth), BF16),
            pltpu.VMEM((LANES // FACTORS, max(lots, NY) * 2 * js, depth), F32),
            pltpu.VMEM((NY, rows, 2 * js, depth), BF16),
            pltpu.VMEM((NY, rows, 2 * js, depth), BF16),
            pltpu.SemaphoreType.DMA((2,)),
        ]
        + sems(NY - 1, NX - 1, NX, NY - 1),
        compiler_params=remote(2),
    )(left.reshape(chunk), right.reshape(chunk), w_exit)
    return aligned.reshape(total, rows, width), (pair.astype(F32) + change).astype(BF16)


def solution(mesh):
    torus = Mesh(mesh.devices.reshape(mesh.shape["groups"], NX, NY, NC), GROUPS_DAP)
    return jax.shard_map(
        shards,
        mesh=torus,
        in_specs=(
            P(GROUPS_DAP, None, None),
            P(GROUPS_DAP, None, None),
            P("groups", None),
        )
        + (P(),) * 7,
        out_specs=(P("groups", DAP, None), P(GROUPS_DAP, None, None)),
        check_vma=False,
    )
```

```python
import jax
import jax.numpy as jnp
from jax import lax
from jax.experimental import pallas as pl
from jax.experimental.pallas import tpu as pltpu
from jax.sharding import Mesh
from jax.sharding import PartitionSpec as P

HEADS = 8
WIDTH = 32
FACTORS = 32
NX, NY, NC = 8, 8, 2
LANES = 128
GROUPS_DAP = ("groups", "dap_0", "dap_1", "dap_2")
DAP = ("dap_0", "dap_1", "dap_2")
MESH = pl.DeviceIdType.MESH
F32, BF16 = jnp.float32, jnp.bfloat16
VMEM = pl.BlockSpec(memory_space=pltpu.VMEM)
LIMIT = 60 * 1024 * 1024
RING_ORDER = (4, 3, 5, 2, 6, 1, 7)


def norm(v):
    center = v - jnp.mean(v, axis=-1, keepdims=True)
    spread = jnp.mean(center * center, axis=-1, keepdims=True)
    return center * lax.rsqrt(spread + 1e-05)


def nt(a, b):
    return lax.dot_general(a, b, (((1,), (1,)), ((), ())), preferred_element_type=F32)


def nn(a, b):
    return jnp.dot(a, b, preferred_element_type=F32)


def here():
    return lax.axis_index("dap_0"), lax.axis_index("dap_1"), lax.axis_index("dap_2")


def place(x, y, c):
    return {"dap_0": x, "dap_1": y, "dap_2": c}


def knock(peers):
    sem = pltpu.get_barrier_semaphore()
    for peer in peers:
        pl.semaphore_signal(sem, inc=1, device_id=peer, device_id_type=MESH)
    return len(peers)


def answered(count):
    pl.semaphore_wait(pltpu.get_barrier_semaphore(), count)


def x_peers(x, y, c):
    return [place((x + k) % NX, y, c) for k in RING_ORDER]


def y_peers(x, y, c):
    return [place(x, (y + k) % NY, c) for k in RING_ORDER]


def push(src, dst, send, recv, peer):
    copy = pltpu.make_async_remote_copy(
        src_ref=src, dst_ref=dst, send_sem=send, recv_sem=recv, device_id=peer, device_id_type=MESH
    )
    copy.start()
    return copy


def keep(src, dst, sem):
    copy = pltpu.make_async_copy(src, dst, sem)
    copy.start()
    return copy


def wide_y(x, y, c):
    out = [(NY * NC - 2, place(x, y, 1 - c), y, 1 - c)]
    for k in RING_ORDER:
        for f in range(NC):
            cc = (c + f) % NC
            yy = (y + k) % NY
            out.append((2 * (k - 1) + f, place(x, yy, cc), yy, cc))
    return out


def wide_x(x, y, c):
    out = [(NX * NC - 2, place(x, y, 1 - c), x, 1 - c)]
    for k in RING_ORDER:
        for f in range(NC):
            cc = (c + f) % NC
            xx = (x + k) % NX
            out.append((2 * (k - 1) + f, place(xx, y, cc), xx, cc))
    return out


def softmax_product(scores, v):
    raised = jnp.exp(scores - jnp.max(scores, axis=-1, keepdims=True)).astype(BF16)
    both = nn(raised, jnp.concatenate([v, jnp.ones_like(v)], axis=-1))
    return both[:, :LANES] / both[:, LANES:]


def head(h):
    per = LANES // WIDTH
    lane = lax.broadcasted_iota(jnp.int32, (1, LANES), 1) // WIDTH
    mask = (lane == h % per).astype(F32).astype(BF16)
    return slice(h // per * LANES, (h // per + 1) * LANES), mask


def merge(parts):
    per = LANES // WIDTH
    tiles = []
    for t in range(HEADS // per):
        total = parts[t * per]
        for e in range(1, per):
            total = total + parts[t * per + e]
        tiles.append(total)
    return jnp.concatenate(tiles, axis=-1)


def row_kernel(
    pair_ref, wb_ref, msa_ref, drop_ref, w_ref, wo_ref, dst,
    own, full, wide, bias, q, k, v, g, raw, res, stage, src, mid0, mid1, keep_sem,
    s0, r0, s1, r1, s2, r2, s3, r3, s4, r4, s5, r5, e0, f0, e1, f1, e2, f2, e3, f3,
):
    seqs, length, width = msa_ref.shape
    pairs = length // 2
    x, y, c = here()
    yc = y * NC + c
    wy, wx = wide_y(x, y, c), wide_x(x, y, c)
    count = knock([p for _, p, _, _ in wy] + [p for _, p, _, _ in wx[1:]])

    zn = norm(pair_ref[...].astype(F32)).astype(BF16)
    rows = nt(wb_ref[...], zn)
    rows = jnp.concatenate([rows[:, :length], rows[:, length:]], axis=0).astype(BF16)
    for t in range(2):
        own[t] = rows[:, t * LANES : (t + 1) * LANES]
    answered(count)

    mine = [keep(own.at[t], full.at[t, x, yc], keep_sem.at[t]) for t in range(2)]
    first0 = [push(own.at[0], full.at[0, x, yc], s0.at[n], r0.at[n], p) for n, p, _, _ in wy]
    first1 = [push(own.at[1], full.at[1, x, yc], s1.at[n], r1.at[n], p) for n, p, _, _ in wx]

    def project(s, carry):
        m1 = norm(msa_ref[s].astype(F32)).astype(BF16)
        q[s] = (nn(m1, w_ref[:, 0:width]) * WIDTH ** (-0.5)).astype(BF16)
        k[s] = nn(m1, w_ref[:, width : 2 * width]).astype(BF16)
        v[s] = nn(m1, w_ref[:, 2 * width : 3 * width]).astype(BF16)
        g[s] = nn(m1, w_ref[:, 3 * width : 4 * width])
        return carry

    lax.fori_loop(0, seqs, project, 0)
    for m in mine:
        m.wait()
    for m in first0:
        m.wait_recv()
    half = pl.ds(c * NY, NY)
    second0 = [
        push(full.at[0, x, half], full.at[0, x, half], s2.at[n - 1], r2.at[n - 1], place((x + n) % NX, y, c))
        for n in RING_ORDER
    ]
    for m in first1:
        m.wait_recv()
    halfx, pair = pl.ds(c * (NX // 2), NX // 2), pl.ds(y * NC, NC)
    second1 = [
        push(full.at[1, halfx, pair], full.at[1, halfx, pair], s3.at[n - 1], r3.at[n - 1], place(x, (y + n) % NY, c))
        for n in RING_ORDER
    ]

    def score(s, carry):
        for h in range(HEADS):
            tile, mask = head(h)
            raw[s, h] = nt(q[s, :, tile] * mask, k[s, :, tile])
        return carry

    lax.fori_loop(0, seqs, score, 0)
    other = place(x, y, 1 - c)
    third = []
    for n in reversed(range(NX - 1)):
        d = RING_ORDER[n]
        second0[n].wait_recv()
        xs = (x + NX - d) % NX
        third.append(push(full.at[0, xs, half], full.at[0, xs, half], s4.at[d - 1], r4.at[d - 1], other))
        second1[n].wait_recv()
        pairs_of = pl.ds(((y + NY - d) % NY) * NC, NC)
        third.append(
            push(full.at[1, halfx, pairs_of], full.at[1, halfx, pairs_of], s5.at[d - 1], r5.at[d - 1], other)
        )
    for m in third:
        m.wait_recv()
    for t in range(2):
        wide[t] = full[t].astype(F32).reshape(length * HEADS, LANES)
    for h in range(HEADS):
        for t in range(2):
            bias[h, :, t * LANES : (t + 1) * LANES] = wide[t, pl.ds(h, length, stride=HEADS), :]

    chunks = src.shape[0]
    group = seqs // chunks
    sent = first0 + first1 + second0 + second1 + third
    hops = []
    for n in range(chunks):

        def one(i, carry):
            s = n * group + i
            parts = []
            for h in range(HEADS):
                tile, mask = head(h)
                parts.append(softmax_product(raw[s, h] + bias[h], v[s, :, tile] * mask))
            gated = (jax.nn.sigmoid(g[s]) * merge(parts)).astype(BF16)
            change = nn(gated, wo_ref[...])
            after = msa_ref[s].astype(F32) + drop_ref[...].astype(F32) * (1.0 / 0.9) * change
            for t in range(2):
                res[t] = after[:, t * LANES : (t + 1) * LANES]
                for r in range(2):
                    stage[t, pl.ds(i * 2 + r, pairs, stride=8), :] = res[t, pl.ds(r, pairs, stride=2), :]
            return carry

        lax.fori_loop(0, group, one, 0)
        for t in range(2):
            value = stage[t].reshape(NX, NY * NC, 8, LANES)[:, :, : group * 2, :]
            src[n, t] = value.astype(BF16)
        h0 = [
            push(src.at[n, 0, (x + d) % NX], mid0.at[n, x], e0.at[n, d - 1], f0.at[n, d - 1], place((x + d) % NX, y, c))
            for d in RING_ORDER
        ]
        h1 = [
            push(src.at[n, 1, :, yy * NC + cc], mid1.at[n, yc], e1.at[n, m], f1.at[n, m], p) for m, p, yy, cc in wy
        ]
        a = keep(src.at[n, 0, x], mid0.at[n, x], keep_sem.at[2 * n])
        b = keep(src.at[n, 1, :, yc], mid1.at[n, yc], keep_sem.at[2 * n + 1])
        hops.append((h0, h1, a, b))
    last = []
    for n, (h0, h1, a, b) in enumerate(hops):
        a.wait()
        b.wait()
        for m in h0:
            m.wait_recv()
        g0 = [
            push(mid0.at[n, :, yy * NC + cc], dst.at[0, :, yc, n], e2.at[n, m], f2.at[n, m], p)
            for m, p, yy, cc in wy
        ]
        a = keep(mid0.at[n, :, yc], dst.at[0, :, yc, n], keep_sem.at[2 * n])
        for m in h1:
            m.wait_recv()
        g1 = [
            push(mid1.at[n, :, (x + d) % NX], dst.at[1, x, :, n], e3.at[n, d - 1], f3.at[n, d - 1], place((x + d) % NX, y, c))
            for d in RING_ORDER
        ]
        b = keep(mid1.at[n, :, x], dst.at[1, x, :, n], keep_sem.at[2 * n + 1])
        last.append((g0, g1, a, b))
        sent += h0 + h1 + g0 + g1
    for g0, g1, a, b in last:
        a.wait()
        b.wait()
        for m in g0 + g1:
            m.wait_recv()
    for m in sent:
        m.wait_send()


def column_kernel(
    in_ref, w_ref, wo_ref, flank_ref, exit_ref, out_ref, change,
    both, q, k, v, g, left, right, lefts, rights, others, prod, wide, diag, tile, arrive, land,
    keep_sem, s0, r0, s1, r1, s2, r2, s3, r3,
):
    width = w_ref.shape[0]
    tokens = out_ref.shape[0]
    seqs = tokens // 2
    x, y, c = here()
    other = place(x, y, 1 - c)
    count = knock(y_peers(x, y, c) + x_peers(x, y, c) + [other])
    for t in range(2):
        both[t] = in_ref[t].astype(F32).reshape(tokens, LANES)
    sent, moves = [], []
    for r in range(2):
        token = jnp.concatenate([both[t, pl.ds(r, seqs, stride=2), :] for t in range(2)], axis=-1)
        m3 = norm(token).astype(BF16)
        q[...] = (nn(m3, w_ref[:, 0:width]) * WIDTH ** (-0.5)).astype(BF16)
        k[...] = nn(m3, w_ref[:, width : 2 * width]).astype(BF16)
        v[...] = nn(m3, w_ref[:, 2 * width : 3 * width]).astype(BF16)
        g[...] = nn(m3, w_ref[:, 3 * width : 4 * width])
        parts = []
        for h in range(HEADS):
            part, mask = head(h)
            parts.append(softmax_product(nt(q[:, part] * mask, k[:, part]), v[:, part] * mask))
        gated = (jax.nn.sigmoid(g[...]) * merge(parts)).astype(BF16)
        after = (token + nn(gated, wo_ref[...])).astype(BF16).astype(F32)
        for t in range(2):
            both[t, pl.ds(r, seqs, stride=2), :] = after[:, t * LANES : (t + 1) * LANES]
        factors = nt(flank_ref[...], norm(after).astype(BF16)).astype(BF16)
        left[r] = factors[:FACTORS]
        right[r] = factors[FACTORS:]
        if r == 0:
            answered(count)
        own = [keep(left.at[r], lefts.at[y, r], keep_sem.at[2 * r]), keep(right.at[r], rights.at[x, r], keep_sem.at[2 * r + 1])]
        fl = [
            push(left.at[r], lefts.at[y, r], s0.at[r, d - 1], r0.at[r, d - 1], place(x, (y + d) % NY, c))
            for d in RING_ORDER
        ]
        fr = [
            push(right.at[r], rights.at[x, r], s1.at[r, d - 1], r1.at[r, d - 1], place((x + d) % NX, y, c))
            for d in RING_ORDER
        ]
        swap = [push(right.at[r], others.at[x, r], s2.at[r, NX - 1], r2.at[r, NX - 1], other)]
        moves.append((own, fl, fr, swap))

    for t in range(2):
        out_ref[:, t * LANES : (t + 1) * LANES] = both[t].astype(BF16)
    depth = exit_ref.shape[1]
    per = LANES // FACTORS
    wide[...] = exit_ref[...].astype(F32)
    diag[...] = jnp.zeros_like(diag)
    for d in range(FACTORS):
        block = wide[pl.ds(d, FACTORS, stride=FACTORS), :].astype(BF16)
        for e in range(per):
            diag[d, e * FACTORS : (e + 1) * FACTORS, e * depth : (e + 1) * depth] = block

    for r, (own, fl, fr, swap) in enumerate(moves):
        for n in reversed(range(NX - 1)):
            d = RING_ORDER[n]
            fr[n].wait_recv()
            xs = (x + NX - d) % NX
            swap.append(push(rights.at[xs, r], others.at[xs, r], s2.at[r, d - 1], r2.at[r, d - 1], other))
        for m in own:
            m.wait()
        for m in fl:
            m.wait_recv()
        sent += fl + fr + swap

    rows = rights.shape[0] * rights.shape[1] * rights.shape[2]
    js = rows // FACTORS
    pitch = FACTORS + 8
    cols = lefts[...].reshape(rows, seqs)
    lots = rows // LANES

    def fill(source, base):
        out = nt(source[...].reshape(rows, seqs), cols) * (1.0 / seqs)
        for n in range(js):
            for u in range(lots):
                at = pl.ds(pl.multiple_of((base + n) * pitch, 8), FACTORS)
                prod[u, at, :] = out[n * FACTORS : (n + 1) * FACTORS, u * LANES : (u + 1) * LANES]

    fill(rights, c * js)
    for _, _, _, swap in moves:
        for m in swap:
            m.wait_recv()
    fill(others, (1 - c) * js)
    for d in range(FACTORS):
        tile[:, d * LANES : (d + 1) * LANES] = jnp.concatenate(
            [prod[u, pl.ds(d, 2 * js, stride=pitch), :] for u in range(lots)], axis=0
        ).astype(BF16)
    update = nn(tile[...], diag[...].reshape(FACTORS * LANES, per * depth))
    for u in range(lots):
        for e in range(per):
            i = u * per + e
            arrive[i // 2, i % 2] = update[u * 2 * js : (u + 1) * 2 * js, e * depth : (e + 1) * depth].astype(BF16)
    own = keep(arrive.at[y], land.at[y], keep_sem.at[0])
    back = [
        push(arrive.at[(y + d) % NY], land.at[y], s3.at[d - 1], r3.at[d - 1], place(x, (y + d) % NY, c))
        for d in RING_ORDER
    ]
    own.wait()
    for m in back:
        m.wait_recv()
    for t in range(2):
        for yy in range(NY):
            prod[t, yy * 2 * js : (yy + 1) * 2 * js, :] = land[yy, t].astype(F32)
            for cc in range(NC):
                for r in range(2):
                    change[t, pl.ds((yy * NC + cc) * 2 + r, NX, stride=NY * NC * 2), :] = prod[
                        t, pl.ds(yy * 2 * js + cc * js + r, NX, stride=2), :
                    ]
    for m in sent + back:
        m.wait_send()


def sems(*counts):
    out = []
    for n in counts:
        n = n if isinstance(n, tuple) else (n,)
        out += [pltpu.SemaphoreType.DMA(n), pltpu.SemaphoreType.DMA(n)]
    return out


def remote(number):
    return pltpu.CompilerParams(collective_id=number, has_side_effects=True, vmem_limit_bytes=LIMIT)


def shards(msa, pair, drop, w_bias, w_row, wo_row, w_col, wo_col, flanks, w_exit):
    seqs, length, width = msa.shape
    rows, _, depth = pair.shape
    wide = NY * NC - 1
    chunks = 2
    part = seqs // chunks * rows
    turned = pl.pallas_call(
        row_kernel,
        out_shape=jax.ShapeDtypeStruct((2, NX, NY * NC, chunks, part, LANES), BF16),
        in_specs=[VMEM] * 6,
        out_specs=VMEM,
        scratch_shapes=[
            pltpu.VMEM((2, rows * HEADS, LANES), BF16),
            pltpu.VMEM((2, NX, NY * NC, rows * HEADS, LANES), BF16),
            pltpu.VMEM((2, length * HEADS, LANES), F32),
            pltpu.VMEM((HEADS, length, length), F32),
            pltpu.VMEM((seqs, length, width), BF16),
            pltpu.VMEM((seqs, length, width), BF16),
            pltpu.VMEM((seqs, length, width), BF16),
            pltpu.VMEM((seqs, length, width), F32),
            pltpu.VMEM((seqs, HEADS, length, length), F32),
            pltpu.VMEM((2, length, LANES), F32),
            pltpu.VMEM((2, length // 2 * 8, LANES), F32),
            pltpu.VMEM((chunks, 2, NX, NY * NC, part, LANES), BF16),
            pltpu.VMEM((chunks, NX, NY * NC, part, LANES), BF16),
            pltpu.VMEM((chunks, NY * NC, NX, part, LANES), BF16),
            pltpu.SemaphoreType.DMA((2 * chunks,)),
        ]
        + sems(wide, wide, NX - 1, NY - 1, NX - 1, NY - 1)
        + sems((chunks, NX - 1), (chunks, wide), (chunks, wide), (chunks, NX - 1)),
        compiler_params=remote(0),
    )(pair.reshape(rows * length, depth), w_bias.T, msa, drop, w_row, wo_row)
    total = seqs * NX * NY * NC
    js = NX * rows
    lots = NY * rows * FACTORS // LANES
    per = LANES // FACTORS
    aligned, change = pl.pallas_call(
        column_kernel,
        out_shape=(
            jax.ShapeDtypeStruct((total * rows, width), BF16),
            jax.ShapeDtypeStruct(pair.shape, F32),
        ),
        in_specs=[VMEM] * 5,
        out_specs=(VMEM,) * 2,
        scratch_shapes=[
            pltpu.VMEM((2, total * rows, LANES), F32),
            pltpu.VMEM((total, width), BF16),
            pltpu.VMEM((total, width), BF16),
            pltpu.VMEM((total, width), BF16),
            pltpu.VMEM((total, width), F32),
            pltpu.VMEM((rows, FACTORS, total), BF16),
            pltpu.VMEM((rows, FACTORS, total), BF16),
            pltpu.VMEM((NY, rows, FACTORS, total), BF16),
            pltpu.VMEM((NX, rows, FACTORS, total), BF16),
            pltpu.VMEM((NX, rows, FACTORS, total), BF16),
            pltpu.VMEM((lots, 2 * js * (FACTORS + 8), LANES), F32),
            pltpu.VMEM(w_exit.shape, F32),
            pltpu.VMEM((FACTORS, LANES, per * depth), BF16),
            pltpu.VMEM((lots * 2 * js, FACTORS * LANES), BF16),
            pltpu.VMEM((NY, rows, 2 * js, depth), BF16),
            pltpu.VMEM((NY, rows, 2 * js, depth), BF16),
            pltpu.SemaphoreType.DMA((4,)),
        ]
        + sems((rows, NY - 1), (rows, NX - 1), (rows, NX), NY - 1),
        compiler_params=remote(1),
    )(turned, w_col, wo_col, flanks.T, w_exit)
    return aligned.reshape(total, rows, width), (pair.astype(F32) + change).astype(BF16)


def solution(mesh):
    torus = Mesh(mesh.devices.reshape(mesh.shape["groups"], NX, NY, NC), GROUPS_DAP)
    return jax.shard_map(
        shards,
        mesh=torus,
        in_specs=(
            P(GROUPS_DAP, None, None),
            P(GROUPS_DAP, None, None),
            P("groups", None),
        )
        + (P(),) * 7,
        out_specs=(P("groups", DAP, None), P(GROUPS_DAP, None, None)),
        check_vma=False,
    )
```

```python
import jax
import jax.numpy as jnp
from jax import lax
from jax.experimental import pallas as pl
from jax.experimental.pallas import tpu as pltpu
from jax.sharding import Mesh
from jax.sharding import PartitionSpec as P

HEADS = 8
WIDTH = 32
FACTORS = 32
NX, NY, NC = 8, 8, 2
LANES = 128
GROUPS_DAP = ("groups", "dap_0", "dap_1", "dap_2")
DAP = ("dap_0", "dap_1", "dap_2")
MESH = pl.DeviceIdType.MESH
F32, BF16 = jnp.float32, jnp.bfloat16
VMEM = pl.BlockSpec(memory_space=pltpu.VMEM)
LIMIT = 60 * 1024 * 1024
RING_ORDER = (4, 3, 5, 2, 6, 1, 7)


def norm(v):
    center = v - jnp.mean(v, axis=-1, keepdims=True)
    spread = jnp.mean(center * center, axis=-1, keepdims=True)
    return center * lax.rsqrt(spread + 1e-05)


def nt(a, b):
    return lax.dot_general(a, b, (((1,), (1,)), ((), ())), preferred_element_type=F32)


def nn(a, b):
    return jnp.dot(a, b, preferred_element_type=F32)


def here():
    return lax.axis_index("dap_0"), lax.axis_index("dap_1"), lax.axis_index("dap_2")


def place(x, y, c):
    return {"dap_0": x, "dap_1": y, "dap_2": c}


def knock(peers):
    sem = pltpu.get_barrier_semaphore()
    for peer in peers:
        pl.semaphore_signal(sem, inc=1, device_id=peer, device_id_type=MESH)
    return len(peers)


def answered(count):
    pl.semaphore_wait(pltpu.get_barrier_semaphore(), count)


def x_peers(x, y, c):
    return [place((x + k) % NX, y, c) for k in RING_ORDER]


def y_peers(x, y, c):
    return [place(x, (y + k) % NY, c) for k in RING_ORDER]


def push(src, dst, send, recv, peer):
    copy = pltpu.make_async_remote_copy(
        src_ref=src, dst_ref=dst, send_sem=send, recv_sem=recv, device_id=peer, device_id_type=MESH
    )
    copy.start()
    return copy


def keep(src, dst, sem):
    copy = pltpu.make_async_copy(src, dst, sem)
    copy.start()
    return copy


def wide_y(x, y, c):
    out = [(NY * NC - 2, place(x, y, 1 - c), y, 1 - c)]
    for k in RING_ORDER:
        for f in range(NC):
            cc = (c + f) % NC
            yy = (y + k) % NY
            out.append((2 * (k - 1) + f, place(x, yy, cc), yy, cc))
    return out


def wide_x(x, y, c):
    out = [(NX * NC - 2, place(x, y, 1 - c), x, 1 - c)]
    for k in RING_ORDER:
        for f in range(NC):
            cc = (c + f) % NC
            xx = (x + k) % NX
            out.append((2 * (k - 1) + f, place(xx, y, cc), xx, cc))
    return out


def softmax_product(scores, v):
    raised = jnp.exp(scores - jnp.max(scores, axis=-1, keepdims=True)).astype(BF16)
    both = nn(raised, jnp.concatenate([v, jnp.ones_like(v)], axis=-1))
    return both[:, :LANES] / both[:, LANES:]


def head(h):
    per = LANES // WIDTH
    lane = lax.broadcasted_iota(jnp.int32, (1, LANES), 1) // WIDTH
    mask = (lane == h % per).astype(F32).astype(BF16)
    return slice(h // per * LANES, (h // per + 1) * LANES), mask


def merge(parts):
    per = LANES // WIDTH
    tiles = []
    for t in range(HEADS // per):
        total = parts[t * per]
        for e in range(1, per):
            total = total + parts[t * per + e]
        tiles.append(total)
    return jnp.concatenate(tiles, axis=-1)


def block_kernel(
    pair_ref, wb_ref, flank_ref, msa_hbm, drop_hbm, w_row_hbm, wo_row_hbm, w_col_hbm, wo_col_hbm, exit_hbm,
    out_ref, change,
    msa_ref, drop_ref, w_ref, wo_ref, w_col, wo_col, exit_ref,
    own, full, wide, bias, q, k, v, g, raw, res, stage, src, mid0, mid1, dst,
    both, q2, k2, v2, g2, left, right, lefts, rights, others, prod, spread, diag, tile, arrive, land,
    load_sem, keep_sem, s0, r0, s1, r1, s2, r2, s3, r3, s4, r4, s5, r5, e0, f0, e1, f1, e2, f2, e3, f3,
    t0, u0, t1, u1, t2, u2, t3, u3,
):
    seqs, length, width = msa_ref.shape
    pairs = length // 2
    x, y, c = here()
    yc = y * NC + c
    wy, wx = wide_y(x, y, c), wide_x(x, y, c)
    count = knock([p for _, p, _, _ in wy] + [p for _, p, _, _ in wx[1:]])
    loads = [
        keep(a, b, load_sem.at[n])
        for n, (a, b) in enumerate(
            [
                (msa_hbm, msa_ref), (w_row_hbm, w_ref), (drop_hbm, drop_ref), (wo_row_hbm, wo_ref),
                (w_col_hbm, w_col), (wo_col_hbm, wo_col), (exit_hbm, exit_ref),
            ]
        )
    ]

    zn = norm(pair_ref[...].astype(F32)).astype(BF16)
    rows = nt(wb_ref[...], zn)
    rows = jnp.concatenate([rows[:, :length], rows[:, length:]], axis=0).astype(BF16)
    for t in range(2):
        own[t] = rows[:, t * LANES : (t + 1) * LANES]
    answered(count)

    mine = [keep(own.at[t], full.at[t, x, yc], keep_sem.at[t]) for t in range(2)]
    first0 = [push(own.at[0], full.at[0, x, yc], s0.at[n], r0.at[n], p) for n, p, _, _ in wy]
    first1 = [push(own.at[1], full.at[1, x, yc], s1.at[n], r1.at[n], p) for n, p, _, _ in wx]

    for m in loads:
        m.wait()

    def project(s, carry):
        m1 = norm(msa_ref[s].astype(F32)).astype(BF16)
        q[s] = (nn(m1, w_ref[:, 0:width]) * WIDTH ** (-0.5)).astype(BF16)
        k[s] = nn(m1, w_ref[:, width : 2 * width]).astype(BF16)
        v[s] = nn(m1, w_ref[:, 2 * width : 3 * width]).astype(BF16)
        g[s] = nn(m1, w_ref[:, 3 * width : 4 * width])
        return carry

    lax.fori_loop(0, seqs, project, 0)
    for m in mine:
        m.wait()
    for m in first0:
        m.wait_recv()
    half = pl.ds(c * NY, NY)
    second0 = [
        push(full.at[0, x, half], full.at[0, x, half], s2.at[n - 1], r2.at[n - 1], place((x + n) % NX, y, c))
        for n in RING_ORDER
    ]
    for m in first1:
        m.wait_recv()
    halfx, pair = pl.ds(c * (NX // 2), NX // 2), pl.ds(y * NC, NC)
    second1 = [
        push(full.at[1, halfx, pair], full.at[1, halfx, pair], s3.at[n - 1], r3.at[n - 1], place(x, (y + n) % NY, c))
        for n in RING_ORDER
    ]

    def score(s, carry):
        for h in range(HEADS):
            tile, mask = head(h)
            raw[s, h] = nt(q[s, :, tile] * mask, k[s, :, tile])
        return carry

    lax.fori_loop(0, seqs, score, 0)
    other = place(x, y, 1 - c)
    third = []
    for n in reversed(range(NX - 1)):
        d = RING_ORDER[n]
        second0[n].wait_recv()
        xs = (x + NX - d) % NX
        third.append(push(full.at[0, xs, half], full.at[0, xs, half], s4.at[d - 1], r4.at[d - 1], other))
        second1[n].wait_recv()
        pairs_of = pl.ds(((y + NY - d) % NY) * NC, NC)
        third.append(
            push(full.at[1, halfx, pairs_of], full.at[1, halfx, pairs_of], s5.at[d - 1], r5.at[d - 1], other)
        )
    for m in third:
        m.wait_recv()
    for t in range(2):
        wide[t] = full[t].astype(F32).reshape(length * HEADS, LANES)
    for h in range(HEADS):
        for t in range(2):
            bias[h, :, t * LANES : (t + 1) * LANES] = wide[t, pl.ds(h, length, stride=HEADS), :]

    chunks = src.shape[0]
    group = seqs // chunks
    sent = first0 + first1 + second0 + second1 + third
    hops = []
    for n in range(chunks):

        def one(i, carry):
            s = n * group + i
            parts = []
            for h in range(HEADS):
                tile, mask = head(h)
                parts.append(softmax_product(raw[s, h] + bias[h], v[s, :, tile] * mask))
            gated = (jax.nn.sigmoid(g[s]) * merge(parts)).astype(BF16)
            change = nn(gated, wo_ref[...])
            after = msa_ref[s].astype(F32) + drop_ref[...].astype(F32) * (1.0 / 0.9) * change
            for t in range(2):
                res[t] = after[:, t * LANES : (t + 1) * LANES]
                for r in range(2):
                    stage[t, pl.ds(i * 2 + r, pairs, stride=8), :] = res[t, pl.ds(r, pairs, stride=2), :]
            return carry

        lax.fori_loop(0, group, one, 0, unroll=2)
        for t in range(2):
            value = stage[t].reshape(NX, NY * NC, 8, LANES)[:, :, : group * 2, :]
            src[n, t] = value.astype(BF16)
        h0 = [
            push(src.at[n, 0, (x + d) % NX], mid0.at[n, x], e0.at[n, d - 1], f0.at[n, d - 1], place((x + d) % NX, y, c))
            for d in RING_ORDER
        ]
        h1 = [
            push(src.at[n, 1, :, yy * NC + cc], mid1.at[n, yc], e1.at[n, m], f1.at[n, m], p) for m, p, yy, cc in wy
        ]
        a = keep(src.at[n, 0, x], mid0.at[n, x], keep_sem.at[2 * n])
        b = keep(src.at[n, 1, :, yc], mid1.at[n, yc], keep_sem.at[2 * n + 1])
        hops.append((h0, h1, a, b))
    last = []
    for n, (h0, h1, a, b) in enumerate(hops):
        a.wait()
        b.wait()
        for m in h0:
            m.wait_recv()
        g0 = [
            push(mid0.at[n, :, yy * NC + cc], dst.at[0, :, yc, n], e2.at[n, m], f2.at[n, m], p)
            for m, p, yy, cc in wy
        ]
        a = keep(mid0.at[n, :, yc], dst.at[0, :, yc, n], keep_sem.at[2 * n])
        for m in h1:
            m.wait_recv()
        g1 = [
            push(mid1.at[n, :, (x + d) % NX], dst.at[1, x, :, n], e3.at[n, d - 1], f3.at[n, d - 1], place((x + d) % NX, y, c))
            for d in RING_ORDER
        ]
        b = keep(mid1.at[n, :, x], dst.at[1, x, :, n], keep_sem.at[2 * n + 1])
        last.append((g0, g1, a, b))
        sent += h0 + h1 + g0 + g1
    for g0, g1, a, b in last:
        a.wait()
        b.wait()
        for m in g0 + g1:
            m.wait_recv()


    seqs, tokens = out_ref.shape[0], 2 * out_ref.shape[0]
    for t in range(2):
        both[t] = dst[t].astype(F32).reshape(tokens, LANES)
    moves = []
    for r in range(2):
        token = jnp.concatenate([both[t, pl.ds(r, seqs, stride=2), :] for t in range(2)], axis=-1)
        m3 = norm(token).astype(BF16)
        q2[...] = (nn(m3, w_col[:, 0:width]) * WIDTH ** (-0.5)).astype(BF16)
        k2[...] = nn(m3, w_col[:, width : 2 * width]).astype(BF16)
        v2[...] = nn(m3, w_col[:, 2 * width : 3 * width]).astype(BF16)
        g2[...] = nn(m3, w_col[:, 3 * width : 4 * width])
        parts = []
        for h in range(HEADS):
            part, mask = head(h)
            parts.append(softmax_product(nt(q2[:, part] * mask, k2[:, part]), v2[:, part] * mask))
        gated = (jax.nn.sigmoid(g2[...]) * merge(parts)).astype(BF16)
        after = (token + nn(gated, wo_col[...])).astype(BF16).astype(F32)
        for t in range(2):
            both[t, pl.ds(r, seqs, stride=2), :] = after[:, t * LANES : (t + 1) * LANES]
        factors = nt(flank_ref[...], norm(after).astype(BF16)).astype(BF16)
        left[r] = factors[:FACTORS]
        right[r] = factors[FACTORS:]
        own = [keep(left.at[r], lefts.at[y, r], keep_sem.at[2 * r]), keep(right.at[r], rights.at[x, r], keep_sem.at[2 * r + 1])]
        fl = [
            push(left.at[r], lefts.at[y, r], t0.at[r, d - 1], u0.at[r, d - 1], place(x, (y + d) % NY, c))
            for d in RING_ORDER
        ]
        fr = [
            push(right.at[r], rights.at[x, r], t1.at[r, d - 1], u1.at[r, d - 1], place((x + d) % NX, y, c))
            for d in RING_ORDER
        ]
        swap = [push(right.at[r], others.at[x, r], t2.at[r, NX - 1], u2.at[r, NX - 1], other)]
        moves.append((own, fl, fr, swap))

    for t in range(2):
        out_ref[:, t] = both[t].reshape(seqs, 2, LANES).astype(BF16)
    depth = exit_ref.shape[1]
    per = LANES // FACTORS
    spread[...] = exit_ref[...].astype(F32)
    diag[...] = jnp.zeros_like(diag)
    for d in range(FACTORS):
        block = spread[pl.ds(d, FACTORS, stride=FACTORS), :].astype(BF16)
        for e in range(per):
            diag[d, e * FACTORS : (e + 1) * FACTORS, e * depth : (e + 1) * depth] = block

    for r, (own, fl, fr, swap) in enumerate(moves):
        for n in reversed(range(NX - 1)):
            d = RING_ORDER[n]
            fr[n].wait_recv()
            xs = (x + NX - d) % NX
            swap.append(push(rights.at[xs, r], others.at[xs, r], t2.at[r, d - 1], u2.at[r, d - 1], other))
        for m in own:
            m.wait()
        for m in fl:
            m.wait_recv()
        sent += fl + fr + swap

    rows = rights.shape[0] * rights.shape[1] * rights.shape[2]
    js = rows // FACTORS
    pitch = FACTORS + 8
    cols = lefts[...].reshape(rows, seqs)
    lots = rows // LANES

    def fill(source, base):
        out = nt(source[...].reshape(rows, seqs), cols) * (1.0 / seqs)
        for n in range(js):
            for u in range(lots):
                at = pl.ds(pl.multiple_of((base + n) * pitch, 8), FACTORS)
                prod[u, at, :] = out[n * FACTORS : (n + 1) * FACTORS, u * LANES : (u + 1) * LANES]

    fill(rights, c * js)
    for _, _, _, swap in moves:
        for m in swap:
            m.wait_recv()
    fill(others, (1 - c) * js)
    for d in range(FACTORS):
        tile[:, d * LANES : (d + 1) * LANES] = jnp.concatenate(
            [prod[u, pl.ds(d, 2 * js, stride=pitch), :] for u in range(lots)], axis=0
        ).astype(BF16)
    update = nn(tile[...], diag[...].reshape(FACTORS * LANES, per * depth))
    for u in range(lots):
        for e in range(per):
            i = u * per + e
            arrive[i // 2, i % 2] = update[u * 2 * js : (u + 1) * 2 * js, e * depth : (e + 1) * depth].astype(BF16)
    own = keep(arrive.at[y], land.at[y], keep_sem.at[0])
    back = [
        push(arrive.at[(y + d) % NY], land.at[y], t3.at[d - 1], u3.at[d - 1], place(x, (y + d) % NY, c))
        for d in RING_ORDER
    ]
    own.wait()
    for m in back:
        m.wait_recv()
    for t in range(2):
        for yy in range(NY):
            prod[t, yy * 2 * js : (yy + 1) * 2 * js, :] = land[yy, t].astype(F32)
            for cc in range(NC):
                for r in range(2):
                    change[t, pl.ds((yy * NC + cc) * 2 + r, NX, stride=NY * NC * 2), :] = prod[
                        t, pl.ds(yy * 2 * js + cc * js + r, NX, stride=2), :
                    ]
    for m in sent + back:
        m.wait_send()


def sems(*counts):
    out = []
    for n in counts:
        n = n if isinstance(n, tuple) else (n,)
        out += [pltpu.SemaphoreType.DMA(n), pltpu.SemaphoreType.DMA(n)]
    return out


def remote(number):
    return pltpu.CompilerParams(collective_id=number, has_side_effects=True, vmem_limit_bytes=LIMIT)


def shards(msa, pair, drop, w_bias, w_row, wo_row, w_col, wo_col, flanks, w_exit):
    seqs, length, width = msa.shape
    rows, _, depth = pair.shape
    wide = NY * NC - 1
    chunks = 2
    part = seqs // chunks * rows
    total = seqs * NX * NY * NC
    js = NX * rows
    lots = NY * rows * FACTORS // LANES
    per = LANES // FACTORS
    later = (msa, drop, w_row, wo_row, w_col, wo_col, w_exit)
    aligned, change = pl.pallas_call(
        block_kernel,
        out_shape=(
            jax.ShapeDtypeStruct((total, width // LANES, rows, LANES), BF16),
            jax.ShapeDtypeStruct(pair.shape, F32),
        ),
        in_specs=[VMEM] * 3 + [pl.BlockSpec(memory_space=pl.ANY)] * len(later),
        out_specs=(VMEM,) * 2,
        scratch_shapes=[pltpu.VMEM(a.shape, a.dtype) for a in later]
        + [
            pltpu.VMEM((2, rows * HEADS, LANES), BF16),
            pltpu.VMEM((2, NX, NY * NC, rows * HEADS, LANES), BF16),
            pltpu.VMEM((2, length * HEADS, LANES), F32),
            pltpu.VMEM((HEADS, length, length), F32),
            pltpu.VMEM((seqs, length, width), BF16),
            pltpu.VMEM((seqs, length, width), BF16),
            pltpu.VMEM((seqs, length, width), BF16),
            pltpu.VMEM((seqs, length, width), F32),
            pltpu.VMEM((seqs, HEADS, length, length), F32),
            pltpu.VMEM((2, length, LANES), F32),
            pltpu.VMEM((2, length // 2 * 8, LANES), F32),
            pltpu.VMEM((chunks, 2, NX, NY * NC, part, LANES), BF16),
            pltpu.VMEM((chunks, NX, NY * NC, part, LANES), BF16),
            pltpu.VMEM((chunks, NY * NC, NX, part, LANES), BF16),
            pltpu.VMEM((2, NX, NY * NC, chunks, part, LANES), BF16),
            pltpu.VMEM((2, total * rows, LANES), F32),
            pltpu.VMEM((total, width), BF16),
            pltpu.VMEM((total, width), BF16),
            pltpu.VMEM((total, width), BF16),
            pltpu.VMEM((total, width), F32),
            pltpu.VMEM((rows, FACTORS, total), BF16),
            pltpu.VMEM((rows, FACTORS, total), BF16),
            pltpu.VMEM((NY, rows, FACTORS, total), BF16),
            pltpu.VMEM((NX, rows, FACTORS, total), BF16),
            pltpu.VMEM((NX, rows, FACTORS, total), BF16),
            pltpu.VMEM((lots, 2 * js * (FACTORS + 8), LANES), F32),
            pltpu.VMEM(w_exit.shape, F32),
            pltpu.VMEM((FACTORS, LANES, per * depth), BF16),
            pltpu.VMEM((lots * 2 * js, FACTORS * LANES), BF16),
            pltpu.VMEM((NY, rows, 2 * js, depth), BF16),
            pltpu.VMEM((NY, rows, 2 * js, depth), BF16),
            pltpu.SemaphoreType.DMA((len(later),)),
            pltpu.SemaphoreType.DMA((2 * chunks,)),
        ]
        + sems(wide, wide, NX - 1, NY - 1, NX - 1, NY - 1)
        + sems((chunks, NX - 1), (chunks, wide), (chunks, wide), (chunks, NX - 1))
        + sems((rows, NY - 1), (rows, NX - 1), (rows, NX), NY - 1),
        compiler_params=remote(0),
    )(pair.reshape(rows * length, depth), w_bias.T, flanks.T, *later)
    return aligned.transpose(0, 2, 1, 3).reshape(total, rows, width), (pair.astype(F32) + change).astype(BF16)


def solution(mesh):
    torus = Mesh(mesh.devices.reshape(mesh.shape["groups"], NX, NY, NC), GROUPS_DAP)
    return jax.shard_map(
        shards,
        mesh=torus,
        in_specs=(
            P(GROUPS_DAP, None, None),
            P(GROUPS_DAP, None, None),
            P("groups", None),
        )
        + (P(),) * 7,
        out_specs=(P("groups", DAP, None), P(GROUPS_DAP, None, None)),
        check_vma=False,
    )
```

```python
import jax
import jax.numpy as jnp
from jax import lax
from jax.experimental import pallas as pl
from jax.experimental.pallas import tpu as pltpu
from jax.sharding import Mesh
from jax.sharding import PartitionSpec as P

HEADS = 8
WIDTH = 32
FACTORS = 32
NX, NY, NC = 8, 8, 2
LANES = 128
GROUPS_DAP = ("groups", "dap_0", "dap_1", "dap_2")
DAP = ("dap_0", "dap_1", "dap_2")
MESH = pl.DeviceIdType.MESH
F32, BF16 = jnp.float32, jnp.bfloat16
VMEM = pl.BlockSpec(memory_space=pltpu.VMEM)
LIMIT = 60 * 1024 * 1024
RING_ORDER = (4, 3, 5, 2, 6, 1, 7)


def norm(v):
    center = v - jnp.mean(v, axis=-1, keepdims=True)
    spread = jnp.mean(center * center, axis=-1, keepdims=True)
    return center * lax.rsqrt(spread + 1e-05)


def nt(a, b):
    return lax.dot_general(a, b, (((1,), (1,)), ((), ())), preferred_element_type=F32)


def nn(a, b):
    return jnp.dot(a, b, preferred_element_type=F32)


def here():
    return lax.axis_index("dap_0"), lax.axis_index("dap_1"), lax.axis_index("dap_2")


def place(x, y, c):
    return {"dap_0": x, "dap_1": y, "dap_2": c}


def knock(peers):
    sem = pltpu.get_barrier_semaphore()
    for peer in peers:
        pl.semaphore_signal(sem, inc=1, device_id=peer, device_id_type=MESH)
    return len(peers)


def answered(count):
    pl.semaphore_wait(pltpu.get_barrier_semaphore(), count)


def x_peers(x, y, c):
    return [place((x + k) % NX, y, c) for k in RING_ORDER]


def y_peers(x, y, c):
    return [place(x, (y + k) % NY, c) for k in RING_ORDER]


def push(src, dst, send, recv, peer):
    copy = pltpu.make_async_remote_copy(
        src_ref=src, dst_ref=dst, send_sem=send, recv_sem=recv, device_id=peer, device_id_type=MESH
    )
    copy.start()
    return copy


def keep(src, dst, sem):
    copy = pltpu.make_async_copy(src, dst, sem)
    copy.start()
    return copy


def near(source, view, me, peer, send, recv):
    return {d: push(source, view(me), send(d - 1), recv(d - 1), peer(d)) for d in (2, 6, 1, 7)}


def far(view, me, peer, send, recv, sent):
    back, ahead = (me + 6) % 8, (me + 2) % 8
    sent[2].wait_recv()
    out = {4: push(view(back, 0), view(back, 0), send(3), recv(3), peer(2))}
    out[3] = push(view(back), view(back), send(2), recv(2), peer(1))
    sent[6].wait_recv()
    out[8] = push(view(ahead, 1), view(ahead, 1), send(7), recv(7), peer(6))
    out[5] = push(view(ahead), view(ahead), send(4), recv(4), peer(7))
    return out


def landed(sent, onward, d):
    if d in (1, 7):
        sent[d].wait_recv()
    elif d in (3, 5):
        onward[d].wait_recv()
    elif d == 4:
        onward[4].wait_recv()
        onward[8].wait_recv()


def wide_y(x, y, c):
    out = [(NY * NC - 2, place(x, y, 1 - c), y, 1 - c)]
    for k in RING_ORDER:
        for f in range(NC):
            cc = (c + f) % NC
            yy = (y + k) % NY
            out.append((2 * (k - 1) + f, place(x, yy, cc), yy, cc))
    return out


def wide_x(x, y, c):
    out = [(NX * NC - 2, place(x, y, 1 - c), x, 1 - c)]
    for k in RING_ORDER:
        for f in range(NC):
            cc = (c + f) % NC
            xx = (x + k) % NX
            out.append((2 * (k - 1) + f, place(xx, y, cc), xx, cc))
    return out


def softmax_product(scores, v):
    raised = jnp.exp(scores - jnp.max(scores, axis=-1, keepdims=True)).astype(BF16)
    both = nn(raised, jnp.concatenate([v, jnp.ones_like(v)], axis=-1))
    return both[:, :LANES] / both[:, LANES:]


def head(h):
    per = LANES // WIDTH
    lane = lax.broadcasted_iota(jnp.int32, (1, LANES), 1) // WIDTH
    mask = (lane == h % per).astype(F32).astype(BF16)
    return slice(h // per * LANES, (h // per + 1) * LANES), mask


def merge(parts):
    per = LANES // WIDTH
    tiles = []
    for t in range(HEADS // per):
        total = parts[t * per]
        for e in range(1, per):
            total = total + parts[t * per + e]
        tiles.append(total)
    return jnp.concatenate(tiles, axis=-1)


def block_kernel(
    pair_ref, wb_ref, flank_ref, msa_hbm, drop_hbm, w_row_hbm, wo_row_hbm, w_col_hbm, wo_col_hbm, exit_hbm,
    out_ref, change,
    msa_ref, drop_ref, w_ref, wo_ref, w_col, wo_col, exit_ref,
    own, full, wide, bias, q, k, v, g, raw, res, stage, src, mid0, mid1, dst,
    both, q2, k2, v2, g2, left, right, lefts, rights, others, prod, spread, diag, tile, arrive, land, total,
    load_sem, keep_sem, s0, r0, s1, r1, s2, r2, s3, r3, s4, r4, s5, r5, e0, f0, e1, f1, e2, f2, e3, f3,
    t0, u0, t1, u1, t2, u2, t3, u3,
):
    seqs, length, width = msa_ref.shape
    pairs = length // 2
    x, y, c = here()
    yc = y * NC + c
    wy, wx = wide_y(x, y, c), wide_x(x, y, c)
    count = knock([p for _, p, _, _ in wy] + [p for _, p, _, _ in wx[1:]])
    loads = [
        keep(a, b, load_sem.at[n])
        for n, (a, b) in enumerate(
            [
                (msa_hbm, msa_ref), (w_row_hbm, w_ref), (drop_hbm, drop_ref), (wo_row_hbm, wo_ref),
                (w_col_hbm, w_col), (wo_col_hbm, wo_col), (exit_hbm, exit_ref),
            ]
        )
    ]

    zn = norm(pair_ref[...].astype(F32)).astype(BF16)
    rows = nt(wb_ref[...], zn)
    rows = jnp.concatenate([rows[:, :length], rows[:, length:]], axis=0).astype(BF16)
    for t in range(2):
        own[t] = rows[:, t * LANES : (t + 1) * LANES]
    answered(count)

    mine = [keep(own.at[t], full.at[t, x, yc], keep_sem.at[t]) for t in range(2)]
    first0 = [push(own.at[0], full.at[0, x, yc], s0.at[n], r0.at[n], p) for n, p, _, _ in wy]
    first1 = [push(own.at[1], full.at[1, x, yc], s1.at[n], r1.at[n], p) for n, p, _, _ in wx]

    for m in loads:
        m.wait()

    def project(s, carry):
        m1 = norm(msa_ref[s].astype(F32)).astype(BF16)
        q[s] = (nn(m1, w_ref[:, 0:width]) * WIDTH ** (-0.5)).astype(BF16)
        k[s] = nn(m1, w_ref[:, width : 2 * width]).astype(BF16)
        v[s] = nn(m1, w_ref[:, 2 * width : 3 * width]).astype(BF16)
        g[s] = nn(m1, w_ref[:, 3 * width : 4 * width])
        return carry

    lax.fori_loop(0, seqs, project, 0)
    for m in mine:
        m.wait()
    for m in first0:
        m.wait_recv()

    def ring_x(at, part=None):
        at_y = pl.ds(c * NY, NY) if part is None else pl.ds(c * NY + part * (NY // 2), NY // 2)
        return full.at[0, at, at_y]

    def ring_y(at, part=None):
        at_x = pl.ds(c * (NX // 2), NX // 2) if part is None else pl.ds(c * (NX // 2) + part * (NX // 4), NX // 4)
        return full.at[1, at_x, pl.ds(at * NC, NC)]

    def to_x(d):
        return place((x + d) % NX, y, c)

    def to_y(d):
        return place(x, (y + d) % NY, c)

    second0 = near(ring_x(x), ring_x, x, to_x, lambda n: s2.at[n], lambda n: r2.at[n])
    for m in first1:
        m.wait_recv()
    second1 = near(ring_y(y), ring_y, y, to_y, lambda n: s3.at[n], lambda n: r3.at[n])

    def score(s, carry):
        for h in range(HEADS):
            tile, mask = head(h)
            raw[s, h] = nt(q[s, :, tile] * mask, k[s, :, tile])
        return carry

    lax.fori_loop(0, seqs, score, 0)
    other = place(x, y, 1 - c)
    third = []
    onward0 = far(ring_x, x, to_x, lambda n: s2.at[n], lambda n: r2.at[n], second0)
    onward1 = far(ring_y, y, to_y, lambda n: s3.at[n], lambda n: r3.at[n], second1)
    for d in (2, 6, 1, 7, 3, 5, 4):
        landed(second0, onward0, d)
        block = ring_x((x + NX - d) % NX)
        third.append(push(block, block, s4.at[d - 1], r4.at[d - 1], other))
        landed(second1, onward1, d)
        block = ring_y((y + NY - d) % NY)
        third.append(push(block, block, s5.at[d - 1], r5.at[d - 1], other))
    for m in third:
        m.wait_recv()
    for t in range(2):
        wide[t] = full[t].astype(F32).reshape(length * HEADS, LANES)
    for h in range(HEADS):
        for t in range(2):
            bias[h, :, t * LANES : (t + 1) * LANES] = wide[t, pl.ds(h, length, stride=HEADS), :]

    chunks = src.shape[0]
    group = seqs // chunks
    sent = first0 + first1 + third
    for some in (second0, onward0, second1, onward1):
        sent += list(some.values())
    hops = []
    for n in range(chunks):

        def one(i, carry):
            s = n * group + i
            parts = []
            for h in range(HEADS):
                tile, mask = head(h)
                parts.append(softmax_product(raw[s, h] + bias[h], v[s, :, tile] * mask))
            gated = (jax.nn.sigmoid(g[s]) * merge(parts)).astype(BF16)
            change = nn(gated, wo_ref[...])
            after = msa_ref[s].astype(F32) + drop_ref[...].astype(F32) * (1.0 / 0.9) * change
            for t in range(2):
                res[t] = after[:, t * LANES : (t + 1) * LANES]
                for r in range(2):
                    stage[t, pl.ds(i * 2 + r, pairs, stride=8), :] = res[t, pl.ds(r, pairs, stride=2), :]
            return carry

        lax.fori_loop(0, group, one, 0, unroll=2)
        for t in range(2):
            value = stage[t].reshape(NX, NY * NC, 8, LANES)[:, :, : group * 2, :]
            src[n, t] = value.astype(BF16)
        h0 = [
            push(src.at[n, 0, (x + d) % NX], mid0.at[n, x], e0.at[n, d - 1], f0.at[n, d - 1], place((x + d) % NX, y, c))
            for d in RING_ORDER
        ]
        h1 = [
            push(src.at[n, 1, :, yy * NC + cc], mid1.at[n, yc], e1.at[n, m], f1.at[n, m], p) for m, p, yy, cc in wy
        ]
        a = keep(src.at[n, 0, x], mid0.at[n, x], keep_sem.at[2 * n])
        b = keep(src.at[n, 1, :, yc], mid1.at[n, yc], keep_sem.at[2 * n + 1])
        hops.append((h0, h1, a, b))
    last = []
    for n, (h0, h1, a, b) in enumerate(hops):
        a.wait()
        b.wait()
        for m in h0:
            m.wait_recv()
        g0 = [
            push(mid0.at[n, :, yy * NC + cc], dst.at[0, :, yc, n], e2.at[n, m], f2.at[n, m], p)
            for m, p, yy, cc in wy
        ]
        a = keep(mid0.at[n, :, yc], dst.at[0, :, yc, n], keep_sem.at[2 * n])
        for m in h1:
            m.wait_recv()
        g1 = [
            push(mid1.at[n, :, (x + d) % NX], dst.at[1, x, :, n], e3.at[n, d - 1], f3.at[n, d - 1], place((x + d) % NX, y, c))
            for d in RING_ORDER
        ]
        b = keep(mid1.at[n, :, x], dst.at[1, x, :, n], keep_sem.at[2 * n + 1])
        last.append((g0, g1, a, b))
        sent += h0 + h1 + g0 + g1
    for g0, g1, a, b in last:
        a.wait()
        b.wait()
        for m in g0 + g1:
            m.wait_recv()


    seqs, tokens = out_ref.shape[0], 2 * out_ref.shape[0]
    for t in range(2):
        both[t] = dst[t].astype(F32).reshape(tokens, LANES)
    moves = []

    def factor_view(ref, r):
        def view(at, part=None):
            if part is None:
                return ref.at[at, r]
            return ref.at[at, r, pl.ds(part * (FACTORS // 2), FACTORS // 2)]

        return view

    for r in range(2):
        token = jnp.concatenate([both[t, pl.ds(r, seqs, stride=2), :] for t in range(2)], axis=-1)
        m3 = norm(token).astype(BF16)
        q2[...] = (nn(m3, w_col[:, 0:width]) * WIDTH ** (-0.5)).astype(BF16)
        k2[...] = nn(m3, w_col[:, width : 2 * width]).astype(BF16)
        v2[...] = nn(m3, w_col[:, 2 * width : 3 * width]).astype(BF16)
        g2[...] = nn(m3, w_col[:, 3 * width : 4 * width])
        parts = []
        for h in range(HEADS):
            part, mask = head(h)
            parts.append(softmax_product(nt(q2[:, part] * mask, k2[:, part]), v2[:, part] * mask))
        gated = (jax.nn.sigmoid(g2[...]) * merge(parts)).astype(BF16)
        after = (token + nn(gated, wo_col[...])).astype(BF16).astype(F32)
        for t in range(2):
            both[t, pl.ds(r, seqs, stride=2), :] = after[:, t * LANES : (t + 1) * LANES]
        factors = nt(flank_ref[...], norm(after).astype(BF16)).astype(BF16)
        left[r] = factors[:FACTORS]
        right[r] = factors[FACTORS:]
        own = [keep(left.at[r], lefts.at[y, r], keep_sem.at[2 * r]), keep(right.at[r], rights.at[x, r], keep_sem.at[2 * r + 1])]
        swap = [push(right.at[r], others.at[x, r], t2.at[r, NX - 1], u2.at[r, NX - 1], other)]
        ways = (factor_view(lefts, r), factor_view(rights, r))
        sems_l = (lambda n, r=r: t0.at[r, n], lambda n, r=r: u0.at[r, n])
        sems_r = (lambda n, r=r: t1.at[r, n], lambda n, r=r: u1.at[r, n])
        fl = near(left.at[r], ways[0], y, to_y, *sems_l)
        fr = near(right.at[r], ways[1], x, to_x, *sems_r)
        moves.append((own, fl, fr, swap, ways, sems_l, sems_r))

    def forward(r):
        _, fl, fr, _, ways, sems_l, sems_r = moves[r]
        return far(ways[0], y, to_y, *sems_l, fl), far(ways[1], x, to_x, *sems_r, fr)

    def hand(r, onward, ds):
        _, fl, fr, swap, _, _, _ = moves[r]
        for d in ds:
            landed(fr, onward[1], d)
            xs = (x + NX - d) % NX
            swap.append(push(rights.at[xs, r], others.at[xs, r], t2.at[r, d - 1], u2.at[r, d - 1], other))
            landed(fl, onward[0], d)

    ahead0 = forward(0)
    for t in range(2):
        out_ref[:, t] = both[t].reshape(seqs, 2, LANES).astype(BF16)
    depth = exit_ref.shape[1]
    per = LANES // FACTORS
    spread[...] = exit_ref[...].astype(F32)
    diag[...] = jnp.zeros_like(diag)
    for d in range(FACTORS):
        block = spread[pl.ds(d, FACTORS, stride=FACTORS), :].astype(BF16)
        for e in range(per):
            diag[d, e * FACTORS : (e + 1) * FACTORS, e * depth : (e + 1) * depth] = block

    hand(0, ahead0, (2, 6, 1, 7))
    ahead1 = forward(1)
    hand(1, ahead1, (2, 6, 1, 7))
    hand(0, ahead0, (3, 5, 4))
    hand(1, ahead1, (3, 5, 4))
    for own, fl, fr, swap, _, _, _ in moves:
        for m in own:
            m.wait()
        sent += list(fl.values()) + list(fr.values()) + swap
    for ways in (ahead0, ahead1):
        for some in ways:
            sent += list(some.values())

    rows = rights.shape[0] * rights.shape[1] * rights.shape[2]
    js = rows // FACTORS
    pitch = FACTORS + 8
    cols = lefts[...].reshape(rows, seqs)
    lots = rows // LANES

    def fill(source, base):
        out = nt(source[...].reshape(rows, seqs), cols) * (1.0 / seqs)
        for n in range(js):
            for u in range(lots):
                at = pl.ds(pl.multiple_of((base + n) * pitch, 8), FACTORS)
                prod[u, at, :] = out[n * FACTORS : (n + 1) * FACTORS, u * LANES : (u + 1) * LANES]

    fill(rights, c * js)
    for move in moves:
        for m in move[3]:
            m.wait_recv()
    fill(others, (1 - c) * js)
    for d in range(FACTORS):
        tile[:, d * LANES : (d + 1) * LANES] = jnp.concatenate(
            [prod[u, pl.ds(d, 2 * js, stride=pitch), :] for u in range(lots)], axis=0
        ).astype(BF16)
    update = nn(tile[...], diag[...].reshape(FACTORS * LANES, per * depth))
    for u in range(lots):
        for e in range(per):
            i = u * per + e
            arrive[i // 2, i % 2] = update[u * 2 * js : (u + 1) * 2 * js, e * depth : (e + 1) * depth].astype(BF16)
    own = keep(arrive.at[y], land.at[y], keep_sem.at[0])
    back = [
        push(arrive.at[(y + d) % NY], land.at[y], t3.at[d - 1], u3.at[d - 1], place(x, (y + d) % NY, c))
        for d in RING_ORDER
    ]
    own.wait()
    for m in back:
        m.wait_recv()
    for t in range(2):
        for yy in range(NY):
            prod[t, yy * 2 * js : (yy + 1) * 2 * js, :] = land[yy, t].astype(F32)
            for cc in range(NC):
                for r in range(2):
                    total[t, pl.ds((yy * NC + cc) * 2 + r, NX, stride=NY * NC * 2), :] = prod[
                        t, pl.ds(yy * 2 * js + cc * js + r, NX, stride=2), :
                    ]
        here_pair = pair_ref[t * length : (t + 1) * length, :].astype(F32)
        change[t] = (here_pair + total[t]).astype(BF16)
    for m in sent + back:
        m.wait_send()


def sems(*counts):
    out = []
    for n in counts:
        n = n if isinstance(n, tuple) else (n,)
        out += [pltpu.SemaphoreType.DMA(n), pltpu.SemaphoreType.DMA(n)]
    return out


def remote(number):
    return pltpu.CompilerParams(collective_id=number, has_side_effects=True, vmem_limit_bytes=LIMIT)


def shards(msa, pair, drop, w_bias, w_row, wo_row, w_col, wo_col, flanks, w_exit):
    seqs, length, width = msa.shape
    rows, _, depth = pair.shape
    wide = NY * NC - 1
    chunks = 2
    part = seqs // chunks * rows
    total = seqs * NX * NY * NC
    js = NX * rows
    lots = NY * rows * FACTORS // LANES
    per = LANES // FACTORS
    later = (msa, drop, w_row, wo_row, w_col, wo_col, w_exit)
    aligned, pair_after = pl.pallas_call(
        block_kernel,
        out_shape=(
            jax.ShapeDtypeStruct((total, width // LANES, rows, LANES), BF16),
            jax.ShapeDtypeStruct(pair.shape, BF16),
        ),
        in_specs=[VMEM] * 3 + [pl.BlockSpec(memory_space=pl.ANY)] * len(later),
        out_specs=(VMEM,) * 2,
        scratch_shapes=[pltpu.VMEM(a.shape, a.dtype) for a in later]
        + [
            pltpu.VMEM((2, rows * HEADS, LANES), BF16),
            pltpu.VMEM((2, NX, NY * NC, rows * HEADS, LANES), BF16),
            pltpu.VMEM((2, length * HEADS, LANES), F32),
            pltpu.VMEM((HEADS, length, length), F32),
            pltpu.VMEM((seqs, length, width), BF16),
            pltpu.VMEM((seqs, length, width), BF16),
            pltpu.VMEM((seqs, length, width), BF16),
            pltpu.VMEM((seqs, length, width), F32),
            pltpu.VMEM((seqs, HEADS, length, length), F32),
            pltpu.VMEM((2, length, LANES), F32),
            pltpu.VMEM((2, length // 2 * 8, LANES), F32),
            pltpu.VMEM((chunks, 2, NX, NY * NC, part, LANES), BF16),
            pltpu.VMEM((chunks, NX, NY * NC, part, LANES), BF16),
            pltpu.VMEM((chunks, NY * NC, NX, part, LANES), BF16),
            pltpu.VMEM((2, NX, NY * NC, chunks, part, LANES), BF16),
            pltpu.VMEM((2, total * rows, LANES), F32),
            pltpu.VMEM((total, width), BF16),
            pltpu.VMEM((total, width), BF16),
            pltpu.VMEM((total, width), BF16),
            pltpu.VMEM((total, width), F32),
            pltpu.VMEM((rows, FACTORS, total), BF16),
            pltpu.VMEM((rows, FACTORS, total), BF16),
            pltpu.VMEM((NY, rows, FACTORS, total), BF16),
            pltpu.VMEM((NX, rows, FACTORS, total), BF16),
            pltpu.VMEM((NX, rows, FACTORS, total), BF16),
            pltpu.VMEM((lots, 2 * js * (FACTORS + 8), LANES), F32),
            pltpu.VMEM(w_exit.shape, F32),
            pltpu.VMEM((FACTORS, LANES, per * depth), BF16),
            pltpu.VMEM((lots * 2 * js, FACTORS * LANES), BF16),
            pltpu.VMEM((NY, rows, 2 * js, depth), BF16),
            pltpu.VMEM((NY, rows, 2 * js, depth), BF16),
            pltpu.VMEM(pair.shape, F32),
            pltpu.SemaphoreType.DMA((len(later),)),
            pltpu.SemaphoreType.DMA((2 * chunks,)),
        ]
        + sems(wide, wide, NX, NY, NX - 1, NY - 1)
        + sems((chunks, NX - 1), (chunks, wide), (chunks, wide), (chunks, NX - 1))
        + sems((rows, NY), (rows, NX), (rows, NX), NY - 1),
        compiler_params=remote(0),
    )(pair.reshape(rows * length, depth), w_bias.T, flanks.T, *later)
    return aligned.transpose(0, 2, 1, 3).reshape(total, rows, width), pair_after


def solution(mesh):
    torus = Mesh(mesh.devices.reshape(mesh.shape["groups"], NX, NY, NC), GROUPS_DAP)
    return jax.shard_map(
        shards,
        mesh=torus,
        in_specs=(
            P(GROUPS_DAP, None, None),
            P(GROUPS_DAP, None, None),
            P("groups", None),
        )
        + (P(),) * 7,
        out_specs=(P("groups", DAP, None), P(GROUPS_DAP, None, None)),
        check_vma=False,
    )
```

```python
import jax
import jax.numpy as jnp
from jax import lax
from jax.experimental import pallas as pl
from jax.experimental.pallas import tpu as pltpu
from jax.sharding import Mesh
from jax.sharding import PartitionSpec as P

HEADS = 8
WIDTH = 32
FACTORS = 32
NX, NY, NC = 8, 8, 2
LANES = 128
GROUPS_DAP = ("groups", "dap_0", "dap_1", "dap_2")
DAP = ("dap_0", "dap_1", "dap_2")
MESH = pl.DeviceIdType.MESH
F32, BF16 = jnp.float32, jnp.bfloat16
VMEM = pl.BlockSpec(memory_space=pltpu.VMEM)
LIMIT = 60 * 1024 * 1024
RING_ORDER = (4, 3, 5, 2, 6, 1, 7)


def norm(v):
    center = v - jnp.mean(v, axis=-1, keepdims=True)
    spread = jnp.mean(center * center, axis=-1, keepdims=True)
    return center * lax.rsqrt(spread + 1e-05)


def nt(a, b):
    return lax.dot_general(a, b, (((1,), (1,)), ((), ())), preferred_element_type=F32)


def nn(a, b):
    return jnp.dot(a, b, preferred_element_type=F32)


def here():
    return lax.axis_index("dap_0"), lax.axis_index("dap_1"), lax.axis_index("dap_2")


def place(x, y, c):
    return {"dap_0": x, "dap_1": y, "dap_2": c}


def knock(peers):
    sem = pltpu.get_barrier_semaphore()
    for peer in peers:
        pl.semaphore_signal(sem, inc=1, device_id=peer, device_id_type=MESH)
    return len(peers)


def answered(count):
    pl.semaphore_wait(pltpu.get_barrier_semaphore(), count)


def x_peers(x, y, c):
    return [place((x + k) % NX, y, c) for k in RING_ORDER]


def y_peers(x, y, c):
    return [place(x, (y + k) % NY, c) for k in RING_ORDER]


def push(src, dst, send, recv, peer):
    copy = pltpu.make_async_remote_copy(
        src_ref=src, dst_ref=dst, send_sem=send, recv_sem=recv, device_id=peer, device_id_type=MESH
    )
    copy.start()
    return copy


def keep(src, dst, sem):
    copy = pltpu.make_async_copy(src, dst, sem)
    copy.start()
    return copy


def near(source, view, me, peer, send, recv):
    return {d: push(source, view(me), send(d - 1), recv(d - 1), peer(d)) for d in (2, 6, 1, 7)}


def far(view, me, peer, send, recv, sent):
    back, ahead = (me + 6) % 8, (me + 2) % 8
    sent[2].wait_recv()
    out = {4: push(view(back, 0), view(back, 0), send(3), recv(3), peer(2))}
    out[3] = push(view(back), view(back), send(2), recv(2), peer(1))
    sent[6].wait_recv()
    out[8] = push(view(ahead, 1), view(ahead, 1), send(7), recv(7), peer(6))
    out[5] = push(view(ahead), view(ahead), send(4), recv(4), peer(7))
    return out


def landed(sent, onward, d):
    if d in (1, 7):
        sent[d].wait_recv()
    elif d in (3, 5):
        onward[d].wait_recv()
    elif d == 4:
        onward[4].wait_recv()
        onward[8].wait_recv()


def wide_y(x, y, c):
    out = [(NY * NC - 2, place(x, y, 1 - c), y, 1 - c)]
    for k in RING_ORDER:
        for f in range(NC):
            cc = (c + f) % NC
            yy = (y + k) % NY
            out.append((2 * (k - 1) + f, place(x, yy, cc), yy, cc))
    return out


def wide_x(x, y, c):
    out = [(NX * NC - 2, place(x, y, 1 - c), x, 1 - c)]
    for k in RING_ORDER:
        for f in range(NC):
            cc = (c + f) % NC
            xx = (x + k) % NX
            out.append((2 * (k - 1) + f, place(xx, y, cc), xx, cc))
    return out


def softmax_product(scores, v):
    raised = jnp.exp(scores - jnp.max(scores, axis=-1, keepdims=True)).astype(BF16)
    both = nn(raised, jnp.concatenate([v, jnp.ones_like(v)], axis=-1))
    return both[:, :LANES] / both[:, LANES:]


def head(h):
    per = LANES // WIDTH
    lane = lax.broadcasted_iota(jnp.int32, (1, LANES), 1) // WIDTH
    mask = (lane == h % per).astype(F32).astype(BF16)
    return slice(h // per * LANES, (h // per + 1) * LANES), mask


def merge(parts):
    per = LANES // WIDTH
    tiles = []
    for t in range(HEADS // per):
        total = parts[t * per]
        for e in range(1, per):
            total = total + parts[t * per + e]
        tiles.append(total)
    return jnp.concatenate(tiles, axis=-1)


def block_kernel(
    pair_hbm, wb_hbm, flank_hbm, msa_hbm, drop_hbm, w_row_hbm, wo_row_hbm, w_col_hbm, wo_col_hbm, exit_hbm,
    out_ref, change,
    pair_ref, wb_ref, flank_ref, msa_ref, drop_ref, w_ref, wo_ref, w_col, wo_col, exit_ref,
    own, full, wide, bias, q, k, v, g, raw, res, stage, src, mid0, mid1, dst,
    both, q2, k2, v2, g2, left, right, lefts, rights, others, prod, spread, diag, tile, arrive, land, total,
    load_sem, keep_sem, s0, r0, s1, r1, s2, r2, s3, r3, s4, r4, s5, r5, e0, f0, e1, f1, e2, f2, e3, f3,
    t0, u0, t1, u1, t2, u2, t3, u3,
):
    seqs, length, width = msa_ref.shape
    pairs = length // 2
    x, y, c = here()
    yc = y * NC + c
    wy, wx = wide_y(x, y, c), wide_x(x, y, c)
    count = knock([p for _, p, _, _ in wy] + [p for _, p, _, _ in wx[1:]])
    loads = [
        keep(a, b, load_sem.at[n])
        for n, (a, b) in enumerate(
            [
                (pair_hbm, pair_ref), (wb_hbm, wb_ref), (flank_hbm, flank_ref), (msa_hbm, msa_ref), (w_row_hbm, w_ref), (drop_hbm, drop_ref), (wo_row_hbm, wo_ref),
                (w_col_hbm, w_col), (wo_col_hbm, wo_col), (exit_hbm, exit_ref),
            ]
        )
    ]

    for m in loads[:2]:
        m.wait()
    zn = norm(pair_ref[...].astype(F32)).astype(BF16)
    rows = nt(wb_ref[...], zn)
    rows = jnp.concatenate([rows[:, :length], rows[:, length:]], axis=0).astype(BF16)
    for t in range(2):
        own[t] = rows[:, t * LANES : (t + 1) * LANES]
    answered(count)

    mine = [keep(own.at[t], full.at[t, x, yc], keep_sem.at[t]) for t in range(2)]
    first0 = [push(own.at[0], full.at[0, x, yc], s0.at[n], r0.at[n], p) for n, p, _, _ in wy]
    first1 = [push(own.at[1], full.at[1, x, yc], s1.at[n], r1.at[n], p) for n, p, _, _ in wx]

    for m in loads[2:]:
        m.wait()

    def project(s, carry):
        m1 = norm(msa_ref[s].astype(F32)).astype(BF16)
        q[s] = (nn(m1, w_ref[:, 0:width]) * WIDTH ** (-0.5)).astype(BF16)
        k[s] = nn(m1, w_ref[:, width : 2 * width]).astype(BF16)
        v[s] = nn(m1, w_ref[:, 2 * width : 3 * width]).astype(BF16)
        g[s] = nn(m1, w_ref[:, 3 * width : 4 * width])
        return carry

    lax.fori_loop(0, seqs, project, 0)
    for m in mine:
        m.wait()
    for m in first0:
        m.wait_recv()

    def ring_x(at, part=None):
        at_y = pl.ds(c * NY, NY) if part is None else pl.ds(c * NY + part * (NY // 2), NY // 2)
        return full.at[0, at, at_y]

    def ring_y(at, part=None):
        at_x = pl.ds(c * (NX // 2), NX // 2) if part is None else pl.ds(c * (NX // 2) + part * (NX // 4), NX // 4)
        return full.at[1, at_x, pl.ds(at * NC, NC)]

    def to_x(d):
        return place((x + d) % NX, y, c)

    def to_y(d):
        return place(x, (y + d) % NY, c)

    second0 = near(ring_x(x), ring_x, x, to_x, lambda n: s2.at[n], lambda n: r2.at[n])
    for m in first1:
        m.wait_recv()
    second1 = near(ring_y(y), ring_y, y, to_y, lambda n: s3.at[n], lambda n: r3.at[n])

    def score(s, carry):
        for h in range(HEADS):
            tile, mask = head(h)
            raw[s, h] = nt(q[s, :, tile] * mask, k[s, :, tile])
        return carry

    lax.fori_loop(0, seqs, score, 0)
    other = place(x, y, 1 - c)
    third = []
    onward0 = far(ring_x, x, to_x, lambda n: s2.at[n], lambda n: r2.at[n], second0)
    onward1 = far(ring_y, y, to_y, lambda n: s3.at[n], lambda n: r3.at[n], second1)
    for d in (2, 6, 1, 7, 3, 5, 4):
        landed(second0, onward0, d)
        block = ring_x((x + NX - d) % NX)
        third.append(push(block, block, s4.at[d - 1], r4.at[d - 1], other))
        landed(second1, onward1, d)
        block = ring_y((y + NY - d) % NY)
        third.append(push(block, block, s5.at[d - 1], r5.at[d - 1], other))
    for m in third:
        m.wait_recv()
    for t in range(2):
        wide[t] = full[t].astype(F32).reshape(length * HEADS, LANES)
    for h in range(HEADS):
        for t in range(2):
            bias[h, :, t * LANES : (t + 1) * LANES] = wide[t, pl.ds(h, length, stride=HEADS), :]

    chunks = src.shape[0]
    group = seqs // chunks
    sent = first0 + first1 + third
    for some in (second0, onward0, second1, onward1):
        sent += list(some.values())
    hops = []
    for n in range(chunks):

        def one(i, carry):
            s = n * group + i
            parts = []
            for h in range(HEADS):
                tile, mask = head(h)
                parts.append(softmax_product(raw[s, h] + bias[h], v[s, :, tile] * mask))
            gated = (jax.nn.sigmoid(g[s]) * merge(parts)).astype(BF16)
            change = nn(gated, wo_ref[...])
            after = msa_ref[s].astype(F32) + drop_ref[...].astype(F32) * (1.0 / 0.9) * change
            for t in range(2):
                res[t] = after[:, t * LANES : (t + 1) * LANES]
                for r in range(2):
                    stage[t, pl.ds(i * 2 + r, pairs, stride=8), :] = res[t, pl.ds(r, pairs, stride=2), :]
            return carry

        lax.fori_loop(0, group, one, 0, unroll=2)
        for t in range(2):
            value = stage[t].reshape(NX, NY * NC, 8, LANES)[:, :, : group * 2, :]
            src[n, t] = value.astype(BF16)
        h0 = [
            push(src.at[n, 0, (x + d) % NX], mid0.at[n, x], e0.at[n, d - 1], f0.at[n, d - 1], place((x + d) % NX, y, c))
            for d in RING_ORDER
        ]
        h1 = [
            push(src.at[n, 1, :, yy * NC + cc], mid1.at[n, yc], e1.at[n, m], f1.at[n, m], p) for m, p, yy, cc in wy
        ]
        a = keep(src.at[n, 0, x], mid0.at[n, x], keep_sem.at[2 * n])
        b = keep(src.at[n, 1, :, yc], mid1.at[n, yc], keep_sem.at[2 * n + 1])
        hops.append((h0, h1, a, b))
    last = []
    for n, (h0, h1, a, b) in enumerate(hops):
        a.wait()
        b.wait()
        for m in h0:
            m.wait_recv()
        g0 = [
            push(mid0.at[n, :, yy * NC + cc], dst.at[0, :, yc, n], e2.at[n, m], f2.at[n, m], p)
            for m, p, yy, cc in wy
        ]
        a = keep(mid0.at[n, :, yc], dst.at[0, :, yc, n], keep_sem.at[2 * n])
        for m in h1:
            m.wait_recv()
        g1 = [
            push(mid1.at[n, :, (x + d) % NX], dst.at[1, x, :, n], e3.at[n, d - 1], f3.at[n, d - 1], place((x + d) % NX, y, c))
            for d in RING_ORDER
        ]
        b = keep(mid1.at[n, :, x], dst.at[1, x, :, n], keep_sem.at[2 * n + 1])
        last.append((g0, g1, a, b))
        sent += h0 + h1 + g0 + g1
    for g0, g1, a, b in last:
        a.wait()
        b.wait()
        for m in g0 + g1:
            m.wait_recv()


    seqs, tokens = out_ref.shape[0], 2 * out_ref.shape[0]
    for t in range(2):
        both[t] = dst[t].astype(F32).reshape(tokens, LANES)
    moves = []

    def factor_view(ref, r):
        def view(at, part=None):
            if part is None:
                return ref.at[at, r]
            return ref.at[at, r, pl.ds(part * (FACTORS // 2), FACTORS // 2)]

        return view

    for r in range(2):
        token = jnp.concatenate([both[t, pl.ds(r, seqs, stride=2), :] for t in range(2)], axis=-1)
        m3 = norm(token).astype(BF16)
        q2[...] = (nn(m3, w_col[:, 0:width]) * WIDTH ** (-0.5)).astype(BF16)
        k2[...] = nn(m3, w_col[:, width : 2 * width]).astype(BF16)
        v2[...] = nn(m3, w_col[:, 2 * width : 3 * width]).astype(BF16)
        g2[...] = nn(m3, w_col[:, 3 * width : 4 * width])
        parts = []
        for h in range(HEADS):
            part, mask = head(h)
            parts.append(softmax_product(nt(q2[:, part] * mask, k2[:, part]), v2[:, part] * mask))
        gated = (jax.nn.sigmoid(g2[...]) * merge(parts)).astype(BF16)
        after = (token + nn(gated, wo_col[...])).astype(BF16).astype(F32)
        for t in range(2):
            both[t, pl.ds(r, seqs, stride=2), :] = after[:, t * LANES : (t + 1) * LANES]
        factors = nt(flank_ref[...], norm(after).astype(BF16)).astype(BF16)
        left[r] = factors[:FACTORS]
        right[r] = factors[FACTORS:]
        own = [keep(left.at[r], lefts.at[y, r], keep_sem.at[2 * r]), keep(right.at[r], rights.at[x, r], keep_sem.at[2 * r + 1])]
        swap = [push(right.at[r], others.at[x, r], t2.at[r, NX - 1], u2.at[r, NX - 1], other)]
        ways = (factor_view(lefts, r), factor_view(rights, r))
        sems_l = (lambda n, r=r: t0.at[r, n], lambda n, r=r: u0.at[r, n])
        sems_r = (lambda n, r=r: t1.at[r, n], lambda n, r=r: u1.at[r, n])
        fl = near(left.at[r], ways[0], y, to_y, *sems_l)
        fr = near(right.at[r], ways[1], x, to_x, *sems_r)
        moves.append((own, fl, fr, swap, ways, sems_l, sems_r))

    def forward(r):
        _, fl, fr, _, ways, sems_l, sems_r = moves[r]
        return far(ways[0], y, to_y, *sems_l, fl), far(ways[1], x, to_x, *sems_r, fr)

    def hand(r, onward, ds):
        _, fl, fr, swap, _, _, _ = moves[r]
        for d in ds:
            landed(fr, onward[1], d)
            xs = (x + NX - d) % NX
            swap.append(push(rights.at[xs, r], others.at[xs, r], t2.at[r, d - 1], u2.at[r, d - 1], other))
            landed(fl, onward[0], d)

    ahead0 = forward(0)
    for t in range(2):
        out_ref[:, t] = both[t].reshape(seqs, 2, LANES).astype(BF16)
    depth = exit_ref.shape[1]
    per = LANES // FACTORS
    spread[...] = exit_ref[...].astype(F32)
    diag[...] = jnp.zeros_like(diag)
    for d in range(FACTORS):
        block = spread[pl.ds(d, FACTORS, stride=FACTORS), :].astype(BF16)
        for e in range(per):
            diag[d, e * FACTORS : (e + 1) * FACTORS, e * depth : (e + 1) * depth] = block

    hand(0, ahead0, (2, 6, 1, 7))
    ahead1 = forward(1)
    hand(1, ahead1, (2, 6, 1, 7))
    hand(0, ahead0, (3, 5, 4))
    hand(1, ahead1, (3, 5, 4))
    for own, fl, fr, swap, _, _, _ in moves:
        for m in own:
            m.wait()
        sent += list(fl.values()) + list(fr.values()) + swap
    for ways in (ahead0, ahead1):
        for some in ways:
            sent += list(some.values())

    rows = rights.shape[0] * rights.shape[1] * rights.shape[2]
    js = rows // FACTORS
    pitch = FACTORS + 8
    cols = lefts[...].reshape(rows, seqs)
    lots = rows // LANES

    back = []
    own = []

    def update(n, source, slot):
        out = nt(source[...].reshape(rows, seqs), cols) * (1.0 / seqs)
        for j in range(js):
            for u in range(lots):
                prod[u, j * pitch : j * pitch + FACTORS, :] = out[
                    j * FACTORS : (j + 1) * FACTORS, u * LANES : (u + 1) * LANES
                ]
        for d in range(FACTORS):
            tile[:, d * LANES : (d + 1) * LANES] = jnp.concatenate(
                [prod[u, pl.ds(d, js, stride=pitch), :] for u in range(lots)], axis=0
            ).astype(BF16)
        add = nn(tile[...], diag[...].reshape(FACTORS * LANES, per * depth))
        for u in range(lots):
            for e in range(per):
                i = u * per + e
                arrive[n, i // 2, i % 2] = add[u * js : (u + 1) * js, e * depth : (e + 1) * depth].astype(BF16)
        own.append(keep(arrive.at[n, y], land.at[slot, y], keep_sem.at[n]))
        for d in RING_ORDER:
            back.append(push(arrive.at[n, (y + d) % NY], land.at[slot, y], t3.at[n, d - 1], u3.at[n, d - 1], to_y(d)))

    update(0, rights, c)
    for move in moves:
        for m in move[3]:
            m.wait_recv()
    update(1, others, 1 - c)
    for m in own:
        m.wait()
    for m in back:
        m.wait_recv()
    for t in range(2):
        for yy in range(NY):
            for cc in range(NC):
                base = (yy * NC + cc) * js
                prod[t, base : base + js, :] = land[cc, yy, t].astype(F32)
                for r in range(2):
                    total[t, pl.ds((yy * NC + cc) * 2 + r, NX, stride=NY * NC * 2), :] = prod[
                        t, pl.ds(base + r, NX, stride=2), :
                    ]
        here_pair = pair_ref[t * length : (t + 1) * length, :].astype(F32)
        change[t] = (here_pair + total[t]).astype(BF16)
    for m in sent + back:
        m.wait_send()


def sems(*counts):
    out = []
    for n in counts:
        n = n if isinstance(n, tuple) else (n,)
        out += [pltpu.SemaphoreType.DMA(n), pltpu.SemaphoreType.DMA(n)]
    return out


def remote(number):
    return pltpu.CompilerParams(collective_id=number, has_side_effects=True, vmem_limit_bytes=LIMIT)


def shards(msa, pair, drop, w_bias, w_row, wo_row, w_col, wo_col, flanks, w_exit):
    seqs, length, width = msa.shape
    rows, _, depth = pair.shape
    wide = NY * NC - 1
    chunks = 2
    part = seqs // chunks * rows
    total = seqs * NX * NY * NC
    js = NX * rows
    lots = NY * rows * FACTORS // LANES
    per = LANES // FACTORS
    later = (pair.reshape(rows * length, depth), w_bias.T, flanks.T, msa, drop, w_row, wo_row, w_col, wo_col, w_exit)
    aligned, pair_after = pl.pallas_call(
        block_kernel,
        out_shape=(
            pltpu.VMEM((total, width // LANES, rows, LANES), BF16),
            pltpu.VMEM(pair.shape, BF16),
        ),
        in_specs=[pl.BlockSpec(memory_space=pl.ANY)] * len(later),
        out_specs=(VMEM,) * 2,
        scratch_shapes=[pltpu.VMEM(a.shape, a.dtype) for a in later]
        + [
            pltpu.VMEM((2, rows * HEADS, LANES), BF16),
            pltpu.VMEM((2, NX, NY * NC, rows * HEADS, LANES), BF16),
            pltpu.VMEM((2, length * HEADS, LANES), F32),
            pltpu.VMEM((HEADS, length, length), F32),
            pltpu.VMEM((seqs, length, width), BF16),
            pltpu.VMEM((seqs, length, width), BF16),
            pltpu.VMEM((seqs, length, width), BF16),
            pltpu.VMEM((seqs, length, width), F32),
            pltpu.VMEM((seqs, HEADS, length, length), F32),
            pltpu.VMEM((2, length, LANES), F32),
            pltpu.VMEM((2, length // 2 * 8, LANES), F32),
            pltpu.VMEM((chunks, 2, NX, NY * NC, part, LANES), BF16),
            pltpu.VMEM((chunks, NX, NY * NC, part, LANES), BF16),
            pltpu.VMEM((chunks, NY * NC, NX, part, LANES), BF16),
            pltpu.VMEM((2, NX, NY * NC, chunks, part, LANES), BF16),
            pltpu.VMEM((2, total * rows, LANES), F32),
            pltpu.VMEM((total, width), BF16),
            pltpu.VMEM((total, width), BF16),
            pltpu.VMEM((total, width), BF16),
            pltpu.VMEM((total, width), F32),
            pltpu.VMEM((rows, FACTORS, total), BF16),
            pltpu.VMEM((rows, FACTORS, total), BF16),
            pltpu.VMEM((NY, rows, FACTORS, total), BF16),
            pltpu.VMEM((NX, rows, FACTORS, total), BF16),
            pltpu.VMEM((NX, rows, FACTORS, total), BF16),
            pltpu.VMEM((lots, js * (FACTORS + 8), LANES), F32),
            pltpu.VMEM(w_exit.shape, F32),
            pltpu.VMEM((FACTORS, LANES, per * depth), BF16),
            pltpu.VMEM((lots * js, FACTORS * LANES), BF16),
            pltpu.VMEM((NC, NY, rows, js, depth), BF16),
            pltpu.VMEM((NC, NY, rows, js, depth), BF16),
            pltpu.VMEM(pair.shape, F32),
            pltpu.SemaphoreType.DMA((len(later),)),
            pltpu.SemaphoreType.DMA((2 * chunks,)),
        ]
        + sems(wide, wide, NX, NY, NX - 1, NY - 1)
        + sems((chunks, NX - 1), (chunks, wide), (chunks, wide), (chunks, NX - 1))
        + sems((rows, NY), (rows, NX), (rows, NX), (NC, NY - 1)),
        compiler_params=remote(0),
    )(*later)
    return aligned.transpose(0, 2, 1, 3).reshape(total, rows, width), pair_after


def solution(mesh):
    torus = Mesh(mesh.devices.reshape(mesh.shape["groups"], NX, NY, NC), GROUPS_DAP)
    return jax.shard_map(
        shards,
        mesh=torus,
        in_specs=(
            P(GROUPS_DAP, None, None),
            P(GROUPS_DAP, None, None),
            P("groups", None),
        )
        + (P(),) * 7,
        out_specs=(P("groups", DAP, None), P(GROUPS_DAP, None, None)),
        check_vma=False,
    )
```

```python
import jax
import jax.numpy as jnp
from jax import lax
from jax.experimental import pallas as pl
from jax.experimental.pallas import tpu as pltpu
from jax.sharding import Mesh
from jax.sharding import PartitionSpec as P

HEADS = 8
WIDTH = 32
FACTORS = 32
NX, NY, NC = 8, 8, 2
LANES = 128
GROUPS_DAP = ("groups", "dap_0", "dap_1", "dap_2")
DAP = ("dap_0", "dap_1", "dap_2")
MESH = pl.DeviceIdType.MESH
F32, BF16 = jnp.float32, jnp.bfloat16
VMEM = pl.BlockSpec(memory_space=pltpu.VMEM)
LIMIT = 60 * 1024 * 1024
RING_ORDER = (4, 3, 5, 2, 6, 1, 7)


def norm(v):
    center = v - jnp.mean(v, axis=-1, keepdims=True)
    spread = jnp.mean(center * center, axis=-1, keepdims=True)
    return center * lax.rsqrt(spread + 1e-05)


def nt(a, b):
    return lax.dot_general(a, b, (((1,), (1,)), ((), ())), preferred_element_type=F32)


def nn(a, b):
    return jnp.dot(a, b, preferred_element_type=F32)


def here():
    return lax.axis_index("dap_0"), lax.axis_index("dap_1"), lax.axis_index("dap_2")


def place(x, y, c):
    return {"dap_0": x, "dap_1": y, "dap_2": c}


def knock(peers):
    sem = pltpu.get_barrier_semaphore()
    for peer in peers:
        pl.semaphore_signal(sem, inc=1, device_id=peer, device_id_type=MESH)
    return len(peers)


def answered(count):
    pl.semaphore_wait(pltpu.get_barrier_semaphore(), count)


def x_peers(x, y, c):
    return [place((x + k) % NX, y, c) for k in RING_ORDER]


def y_peers(x, y, c):
    return [place(x, (y + k) % NY, c) for k in RING_ORDER]


def push(src, dst, send, recv, peer):
    copy = pltpu.make_async_remote_copy(
        src_ref=src, dst_ref=dst, send_sem=send, recv_sem=recv, device_id=peer, device_id_type=MESH
    )
    copy.start()
    return copy


def keep(src, dst, sem):
    copy = pltpu.make_async_copy(src, dst, sem)
    copy.start()
    return copy


def near(source, view, me, peer, send, recv):
    return {d: push(source, view(me), send(d - 1), recv(d - 1), peer(d)) for d in (2, 6, 1, 7)}


def far(view, me, peer, send, recv, sent):
    back, ahead = (me + 6) % 8, (me + 2) % 8
    sent[2].wait_recv()
    out = {4: push(view(back, 0), view(back, 0), send(3), recv(3), peer(2))}
    out[3] = push(view(back), view(back), send(2), recv(2), peer(1))
    sent[6].wait_recv()
    out[8] = push(view(ahead, 1), view(ahead, 1), send(7), recv(7), peer(6))
    out[5] = push(view(ahead), view(ahead), send(4), recv(4), peer(7))
    return out


def landed(sent, onward, d):
    if d in (1, 7):
        sent[d].wait_recv()
    elif d in (3, 5):
        onward[d].wait_recv()
    elif d == 4:
        onward[4].wait_recv()
        onward[8].wait_recv()


def wide_y(x, y, c):
    out = [(NY * NC - 2, place(x, y, 1 - c), y, 1 - c)]
    for k in RING_ORDER:
        for f in range(NC):
            cc = (c + f) % NC
            yy = (y + k) % NY
            out.append((2 * (k - 1) + f, place(x, yy, cc), yy, cc))
    return out


def wide_x(x, y, c):
    out = [(NX * NC - 2, place(x, y, 1 - c), x, 1 - c)]
    for k in RING_ORDER:
        for f in range(NC):
            cc = (c + f) % NC
            xx = (x + k) % NX
            out.append((2 * (k - 1) + f, place(xx, y, cc), xx, cc))
    return out


def softmax_product(scores, v):
    raised = jnp.exp(scores - jnp.max(scores, axis=-1, keepdims=True)).astype(BF16)
    both = nn(raised, jnp.concatenate([v, jnp.ones_like(v)], axis=-1))
    return both[:, :LANES] / both[:, LANES:]


def head(h):
    per = LANES // WIDTH
    lane = lax.broadcasted_iota(jnp.int32, (1, LANES), 1) // WIDTH
    mask = (lane == h % per).astype(F32).astype(BF16)
    return slice(h // per * LANES, (h // per + 1) * LANES), mask


def merge(parts):
    per = LANES // WIDTH
    tiles = []
    for t in range(HEADS // per):
        total = parts[t * per]
        for e in range(1, per):
            total = total + parts[t * per + e]
        tiles.append(total)
    return jnp.concatenate(tiles, axis=-1)


def block_kernel(
    pair_hbm, wb_hbm, flank_hbm, msa_hbm, drop_hbm, w_row_hbm, wo_row_hbm, w_col_hbm, wo_col_hbm, exit_hbm,
    out_ref, change,
    pair_ref, wb_ref, flank_ref, msa_ref, drop_ref, w_ref, wo_ref, w_col, wo_col, exit_ref,
    own, full, wide, bias, q, k, v, g, raw, res, stage, src, mid0, mid1, dst,
    both, q2, k2, v2, g2, left, right, lefts, rights, others, prod, spread, diag, tile, arrive, land, total,
    load_sem, keep_sem, s0, r0, s1, r1, s2, r2, s3, r3, s4, r4, s5, r5, e0, f0, e1, f1, e2, f2, e3, f3,
    t0, u0, t1, u1, t2, u2, t3, u3,
):
    seqs, length, width = msa_ref.shape
    pairs = length // 2
    x, y, c = here()
    yc = y * NC + c
    wy, wx = wide_y(x, y, c), wide_x(x, y, c)
    count = knock([p for _, p, _, _ in wy] + [p for _, p, _, _ in wx[1:]])
    loads = [
        keep(a, b, load_sem.at[n])
        for n, (a, b) in enumerate(
            [
                (pair_hbm, pair_ref), (wb_hbm, wb_ref), (flank_hbm, flank_ref), (msa_hbm, msa_ref), (w_row_hbm, w_ref), (drop_hbm, drop_ref), (wo_row_hbm, wo_ref),
                (w_col_hbm, w_col), (wo_col_hbm, wo_col), (exit_hbm, exit_ref),
            ]
        )
    ]

    for m in loads[:2]:
        m.wait()
    zn = norm(pair_ref[...].astype(F32)).astype(BF16)
    rows = nt(wb_ref[...], zn)
    rows = jnp.concatenate([rows[:, :length], rows[:, length:]], axis=0).astype(BF16)
    for t in range(2):
        own[t] = rows[:, t * LANES : (t + 1) * LANES]
    answered(count)

    mine = [keep(own.at[t], full.at[t, x, yc], keep_sem.at[t]) for t in range(2)]
    first0 = [push(own.at[0], full.at[0, x, yc], s0.at[n], r0.at[n], p) for n, p, _, _ in wy]
    first1 = [push(own.at[1], full.at[1, x, yc], s1.at[n], r1.at[n], p) for n, p, _, _ in wx]

    for m in loads[2:]:
        m.wait()

    def project(s, carry):
        m1 = norm(msa_ref[s].astype(F32)).astype(BF16)
        q[s] = (nn(m1, w_ref[:, 0:width]) * WIDTH ** (-0.5)).astype(BF16)
        k[s] = nn(m1, w_ref[:, width : 2 * width]).astype(BF16)
        v[s] = nn(m1, w_ref[:, 2 * width : 3 * width]).astype(BF16)
        g[s] = nn(m1, w_ref[:, 3 * width : 4 * width])
        return carry

    lax.fori_loop(0, seqs, project, 0, unroll=2)
    for m in mine:
        m.wait()
    for m in first0:
        m.wait_recv()

    def ring_x(at, part=None):
        at_y = pl.ds(c * NY, NY) if part is None else pl.ds(c * NY + part * (NY // 2), NY // 2)
        return full.at[0, at, at_y]

    def ring_y(at, part=None):
        at_x = pl.ds(c * (NX // 2), NX // 2) if part is None else pl.ds(c * (NX // 2) + part * (NX // 4), NX // 4)
        return full.at[1, at_x, pl.ds(at * NC, NC)]

    def to_x(d):
        return place((x + d) % NX, y, c)

    def to_y(d):
        return place(x, (y + d) % NY, c)

    second0 = near(ring_x(x), ring_x, x, to_x, lambda n: s2.at[n], lambda n: r2.at[n])
    for m in first1:
        m.wait_recv()
    second1 = near(ring_y(y), ring_y, y, to_y, lambda n: s3.at[n], lambda n: r3.at[n])

    def score(s, carry):
        for h in range(HEADS):
            tile, mask = head(h)
            raw[s, h] = nt(q[s, :, tile] * mask, k[s, :, tile])
        return carry

    lax.fori_loop(0, seqs // 2, score, 0, unroll=2)
    other = place(x, y, 1 - c)
    third = []
    onward0 = far(ring_x, x, to_x, lambda n: s2.at[n], lambda n: r2.at[n], second0)
    onward1 = far(ring_y, y, to_y, lambda n: s3.at[n], lambda n: r3.at[n], second1)

    def hand_bias(ds):
        for d in ds:
            landed(second0, onward0, d)
            block = ring_x((x + NX - d) % NX)
            third.append(push(block, block, s4.at[d - 1], r4.at[d - 1], other))
            landed(second1, onward1, d)
            block = ring_y((y + NY - d) % NY)
            third.append(push(block, block, s5.at[d - 1], r5.at[d - 1], other))

    hand_bias((2, 6, 1, 7))
    lax.fori_loop(seqs // 2, seqs, score, 0, unroll=2)
    hand_bias((3, 5, 4))
    for m in third:
        m.wait_recv()
    for t in range(2):
        wide[t] = full[t].astype(F32).reshape(length * HEADS, LANES)
    for h in range(HEADS):
        for t in range(2):
            bias[h, :, t * LANES : (t + 1) * LANES] = wide[t, pl.ds(h, length, stride=HEADS), :]

    chunks = src.shape[0]
    group = seqs // chunks
    sent = first0 + first1 + third
    for some in (second0, onward0, second1, onward1):
        sent += list(some.values())
    hops = []
    for n in range(chunks):

        def one(i, carry):
            s = n * group + i
            parts = []
            for h in range(HEADS):
                tile, mask = head(h)
                parts.append(softmax_product(raw[s, h] + bias[h], v[s, :, tile] * mask))
            gated = (jax.nn.sigmoid(g[s]) * merge(parts)).astype(BF16)
            change = nn(gated, wo_ref[...])
            after = msa_ref[s].astype(F32) + drop_ref[...].astype(F32) * (1.0 / 0.9) * change
            for t in range(2):
                res[t] = after[:, t * LANES : (t + 1) * LANES]
                for r in range(2):
                    stage[t, pl.ds(i * 2 + r, pairs, stride=8), :] = res[t, pl.ds(r, pairs, stride=2), :]
            return carry

        lax.fori_loop(0, group, one, 0, unroll=2)
        for t in range(2):
            value = stage[t].reshape(NX, NY * NC, 8, LANES)[:, :, : group * 2, :]
            src[n, t] = value.astype(BF16)
        h0 = [
            push(src.at[n, 0, (x + d) % NX], mid0.at[n, x], e0.at[n, d - 1], f0.at[n, d - 1], place((x + d) % NX, y, c))
            for d in RING_ORDER
        ]
        h1 = [
            push(src.at[n, 1, :, yy * NC + cc], mid1.at[n, yc], e1.at[n, m], f1.at[n, m], p) for m, p, yy, cc in wy
        ]
        a = keep(src.at[n, 0, x], mid0.at[n, x], keep_sem.at[2 * n])
        b = keep(src.at[n, 1, :, yc], mid1.at[n, yc], keep_sem.at[2 * n + 1])
        hops.append((h0, h1, a, b))
    last = []
    for n, (h0, h1, a, b) in enumerate(hops):
        a.wait()
        b.wait()
        for m in h0:
            m.wait_recv()
        g0 = [
            push(mid0.at[n, :, yy * NC + cc], dst.at[0, :, yc, n], e2.at[n, m], f2.at[n, m], p)
            for m, p, yy, cc in wy
        ]
        a = keep(mid0.at[n, :, yc], dst.at[0, :, yc, n], keep_sem.at[2 * n])
        for m in h1:
            m.wait_recv()
        g1 = [
            push(mid1.at[n, :, (x + d) % NX], dst.at[1, x, :, n], e3.at[n, d - 1], f3.at[n, d - 1], place((x + d) % NX, y, c))
            for d in RING_ORDER
        ]
        b = keep(mid1.at[n, :, x], dst.at[1, x, :, n], keep_sem.at[2 * n + 1])
        last.append((g0, g1, a, b))
        sent += h0 + h1 + g0 + g1
    for g0, g1, a, b in last:
        a.wait()
        b.wait()
        for m in g0 + g1:
            m.wait_recv()


    seqs, tokens = out_ref.shape[0], 2 * out_ref.shape[0]
    for t in range(2):
        both[t] = dst[t].astype(F32).reshape(tokens, LANES)
    moves = []

    def factor_view(ref, r):
        def view(at, part=None):
            if part is None:
                return ref.at[at, r]
            return ref.at[at, r, pl.ds(part * (FACTORS // 2), FACTORS // 2)]

        return view

    for r in range(2):
        token = jnp.concatenate([both[t, pl.ds(r, seqs, stride=2), :] for t in range(2)], axis=-1)
        m3 = norm(token).astype(BF16)
        q2[...] = (nn(m3, w_col[:, 0:width]) * WIDTH ** (-0.5)).astype(BF16)
        k2[...] = nn(m3, w_col[:, width : 2 * width]).astype(BF16)
        v2[...] = nn(m3, w_col[:, 2 * width : 3 * width]).astype(BF16)
        g2[...] = nn(m3, w_col[:, 3 * width : 4 * width])
        parts = []
        for h in range(HEADS):
            part, mask = head(h)
            parts.append(softmax_product(nt(q2[:, part] * mask, k2[:, part]), v2[:, part] * mask))
        gated = (jax.nn.sigmoid(g2[...]) * merge(parts)).astype(BF16)
        after = (token + nn(gated, wo_col[...])).astype(BF16).astype(F32)
        for t in range(2):
            both[t, pl.ds(r, seqs, stride=2), :] = after[:, t * LANES : (t + 1) * LANES]
        factors = nt(flank_ref[...], norm(after).astype(BF16)).astype(BF16)
        left[r] = factors[:FACTORS]
        right[r] = factors[FACTORS:]
        own = [keep(left.at[r], lefts.at[y, r], keep_sem.at[2 * r]), keep(right.at[r], rights.at[x, r], keep_sem.at[2 * r + 1])]
        swap = [push(right.at[r], others.at[x, r], t2.at[r, NX - 1], u2.at[r, NX - 1], other)]
        ways = (factor_view(lefts, r), factor_view(rights, r))
        sems_l = (lambda n, r=r: t0.at[r, n], lambda n, r=r: u0.at[r, n])
        sems_r = (lambda n, r=r: t1.at[r, n], lambda n, r=r: u1.at[r, n])
        fl = near(left.at[r], ways[0], y, to_y, *sems_l)
        fr = near(right.at[r], ways[1], x, to_x, *sems_r)
        moves.append((own, fl, fr, swap, ways, sems_l, sems_r))

    def forward(r):
        _, fl, fr, _, ways, sems_l, sems_r = moves[r]
        return far(ways[0], y, to_y, *sems_l, fl), far(ways[1], x, to_x, *sems_r, fr)

    def hand(r, onward, ds):
        _, fl, fr, swap, _, _, _ = moves[r]
        for d in ds:
            landed(fr, onward[1], d)
            xs = (x + NX - d) % NX
            swap.append(push(rights.at[xs, r], others.at[xs, r], t2.at[r, d - 1], u2.at[r, d - 1], other))
            landed(fl, onward[0], d)

    ahead0 = forward(0)
    for t in range(2):
        out_ref[:, t] = both[t].reshape(seqs, 2, LANES).astype(BF16)
    depth = exit_ref.shape[1]
    per = LANES // FACTORS
    spread[...] = exit_ref[...].astype(F32)
    diag[...] = jnp.zeros_like(diag)
    for d in range(FACTORS):
        block = spread[pl.ds(d, FACTORS, stride=FACTORS), :].astype(BF16)
        for e in range(per):
            diag[d, e * FACTORS : (e + 1) * FACTORS, e * depth : (e + 1) * depth] = block

    hand(0, ahead0, (2, 6, 1, 7))
    ahead1 = forward(1)
    hand(1, ahead1, (2, 6, 1, 7))
    hand(0, ahead0, (3, 5, 4))
    hand(1, ahead1, (3, 5, 4))
    for own, fl, fr, swap, _, _, _ in moves:
        for m in own:
            m.wait()
        sent += list(fl.values()) + list(fr.values()) + swap
    for ways in (ahead0, ahead1):
        for some in ways:
            sent += list(some.values())

    rows = rights.shape[0] * rights.shape[1] * rights.shape[2]
    js = rows // FACTORS
    pitch = FACTORS + 8
    cols = lefts[...].reshape(rows, seqs)
    lots = rows // LANES

    back = []
    own = []

    def update(n, source, slot):
        out = nt(source[...].reshape(rows, seqs), cols) * (1.0 / seqs)
        for j in range(js):
            for u in range(lots):
                prod[u, j * pitch : j * pitch + FACTORS, :] = out[
                    j * FACTORS : (j + 1) * FACTORS, u * LANES : (u + 1) * LANES
                ]
        for d in range(FACTORS):
            tile[:, d * LANES : (d + 1) * LANES] = jnp.concatenate(
                [prod[u, pl.ds(d, js, stride=pitch), :] for u in range(lots)], axis=0
            ).astype(BF16)
        add = nn(tile[...], diag[...].reshape(FACTORS * LANES, per * depth))
        for u in range(lots):
            for e in range(per):
                i = u * per + e
                arrive[n, i // 2, i % 2] = add[u * js : (u + 1) * js, e * depth : (e + 1) * depth].astype(BF16)
        own.append(keep(arrive.at[n, y], land.at[slot, y], keep_sem.at[n]))
        for d in RING_ORDER:
            back.append(push(arrive.at[n, (y + d) % NY], land.at[slot, y], t3.at[n, d - 1], u3.at[n, d - 1], to_y(d)))

    update(0, rights, c)
    for move in moves:
        for m in move[3]:
            m.wait_recv()
    update(1, others, 1 - c)
    for m in own:
        m.wait()
    for m in back:
        m.wait_recv()
    for t in range(2):
        for yy in range(NY):
            for cc in range(NC):
                base = (yy * NC + cc) * js
                prod[t, base : base + js, :] = land[cc, yy, t].astype(F32)
                for r in range(2):
                    total[t, pl.ds((yy * NC + cc) * 2 + r, NX, stride=NY * NC * 2), :] = prod[
                        t, pl.ds(base + r, NX, stride=2), :
                    ]
        here_pair = pair_ref[t * length : (t + 1) * length, :].astype(F32)
        change[t] = (here_pair + total[t]).astype(BF16)
    for m in sent + back:
        m.wait_send()


def sems(*counts):
    out = []
    for n in counts:
        n = n if isinstance(n, tuple) else (n,)
        out += [pltpu.SemaphoreType.DMA(n), pltpu.SemaphoreType.DMA(n)]
    return out


def remote(number):
    return pltpu.CompilerParams(collective_id=number, has_side_effects=True, vmem_limit_bytes=LIMIT)


def shards(msa, pair, drop, w_bias, w_row, wo_row, w_col, wo_col, flanks, w_exit):
    seqs, length, width = msa.shape
    rows, _, depth = pair.shape
    wide = NY * NC - 1
    chunks = 2
    part = seqs // chunks * rows
    total = seqs * NX * NY * NC
    js = NX * rows
    lots = NY * rows * FACTORS // LANES
    per = LANES // FACTORS
    later = (pair.reshape(rows * length, depth), w_bias.T, flanks.T, msa, drop, w_row, wo_row, w_col, wo_col, w_exit)
    aligned, pair_after = pl.pallas_call(
        block_kernel,
        out_shape=(
            pltpu.VMEM((total, width // LANES, rows, LANES), BF16),
            pltpu.VMEM(pair.shape, BF16),
        ),
        in_specs=[pl.BlockSpec(memory_space=pl.ANY)] * len(later),
        out_specs=(VMEM,) * 2,
        scratch_shapes=[pltpu.VMEM(a.shape, a.dtype) for a in later]
        + [
            pltpu.VMEM((2, rows * HEADS, LANES), BF16),
            pltpu.VMEM((2, NX, NY * NC, rows * HEADS, LANES), BF16),
            pltpu.VMEM((2, length * HEADS, LANES), F32),
            pltpu.VMEM((HEADS, length, length), F32),
            pltpu.VMEM((seqs, length, width), BF16),
            pltpu.VMEM((seqs, length, width), BF16),
            pltpu.VMEM((seqs, length, width), BF16),
            pltpu.VMEM((seqs, length, width), F32),
            pltpu.VMEM((seqs, HEADS, length, length), F32),
            pltpu.VMEM((2, length, LANES), F32),
            pltpu.VMEM((2, length // 2 * 8, LANES), F32),
            pltpu.VMEM((chunks, 2, NX, NY * NC, part, LANES), BF16),
            pltpu.VMEM((chunks, NX, NY * NC, part, LANES), BF16),
            pltpu.VMEM((chunks, NY * NC, NX, part, LANES), BF16),
            pltpu.VMEM((2, NX, NY * NC, chunks, part, LANES), BF16),
            pltpu.VMEM((2, total * rows, LANES), F32),
            pltpu.VMEM((total, width), BF16),
            pltpu.VMEM((total, width), BF16),
            pltpu.VMEM((total, width), BF16),
            pltpu.VMEM((total, width), F32),
            pltpu.VMEM((rows, FACTORS, total), BF16),
            pltpu.VMEM((rows, FACTORS, total), BF16),
            pltpu.VMEM((NY, rows, FACTORS, total), BF16),
            pltpu.VMEM((NX, rows, FACTORS, total), BF16),
            pltpu.VMEM((NX, rows, FACTORS, total), BF16),
            pltpu.VMEM((lots, js * (FACTORS + 8), LANES), F32),
            pltpu.VMEM(w_exit.shape, F32),
            pltpu.VMEM((FACTORS, LANES, per * depth), BF16),
            pltpu.VMEM((lots * js, FACTORS * LANES), BF16),
            pltpu.VMEM((NC, NY, rows, js, depth), BF16),
            pltpu.VMEM((NC, NY, rows, js, depth), BF16),
            pltpu.VMEM(pair.shape, F32),
            pltpu.SemaphoreType.DMA((len(later),)),
            pltpu.SemaphoreType.DMA((2 * chunks,)),
        ]
        + sems(wide, wide, NX, NY, NX - 1, NY - 1)
        + sems((chunks, NX - 1), (chunks, wide), (chunks, wide), (chunks, NX - 1))
        + sems((rows, NY), (rows, NX), (rows, NX), (NC, NY - 1)),
        compiler_params=remote(0),
    )(*later)
    return aligned.transpose(0, 2, 1, 3).reshape(total, rows, width), pair_after


def solution(mesh):
    torus = Mesh(mesh.devices.reshape(mesh.shape["groups"], NX, NY, NC), GROUPS_DAP)
    return jax.shard_map(
        shards,
        mesh=torus,
        in_specs=(
            P(GROUPS_DAP, None, None),
            P(GROUPS_DAP, None, None),
            P("groups", None),
        )
        + (P(),) * 7,
        out_specs=(P("groups", DAP, None), P(GROUPS_DAP, None, None)),
        check_vma=False,
    )
```
